256 devices in a mesh: seq: 128 (over z_lo, y, x, core), head: 2 (over z_hi).
Axes of the slice: x: 4, y: 4, z: 8 (z_hi: 2, z_lo: 4; z = z_hi * 4 + z_lo), core: 2. Of those that a mesh axis runs over, the one named last changes fastest.
Arguments:
- queries: bfloat16 [16384, 2048], P('seq', 'head'), may hold values from -144 to 144
- keys: bfloat16 [16384, 2048], P('seq', 'head'), may hold values from -4 to 4
- values: bfloat16 [16384, 2048], P('seq', 'head'), may hold values from -6 to 6
- grad_out: bfloat16 [16384, 2048], P('seq', 'head'), may hold values from -6 to 6
- bias_table: float32 [32, 128], P('head'), may hold values from -5 to 5
- bucket_ids: int32 [128, 4, 256], P('seq'), may hold values from 0 to 127
- block_mask: int32 [128, 4], P('seq'), may hold values 0 or 1
Outputs:
- grad_queries: bfloat16 [16384, 2048], P('seq', 'head')
- grad_keys: bfloat16 [16384, 2048], P('seq', 'head')
- grad_values: bfloat16 [16384, 2048], P('seq', 'head')
- grad_bias: float32 [32, 128], replicated
The draws below stay inside these ranges and needn't reach their ends.
All inputs are finite; a program needn't handle non-finite values. No bound on the sum of `block_mask` on one device may be relied on, other than what follows from the above.
Results may differ from the reference program's by a relative error of at most 0.005.
Values may be sent and summed in bfloat16 or wider, within the bound.
A program may use at most 64 MiB of HBM per device.

```python
import jax
import jax.numpy as jnp
from jax import lax

HEADS = 32
HEAD_DIM = 64
BUCKETS = 128
TOK_DEV = 128
SPAN = 4
BLOCKS = 128
TOKENS = 16384
N_SEQ = 128


def drawn_pair(key):
    width = HEADS * HEAD_DIM
    base_keys = jnp.clip(jax.random.normal(jax.random.fold_in(key, 11), (TOKENS, width), jnp.float32), -4.0, 4.0)
    base_queries = jnp.clip(jax.random.normal(jax.random.fold_in(key, 12), (TOKENS, width), jnp.float32), -4.0, 4.0)
    return (base_queries, base_keys)


def draw_queries(key, part):
    return drawn_pair(key)[0].astype(jnp.bfloat16)


def draw_keys(key, part):
    return drawn_pair(key)[1].astype(jnp.bfloat16)


def set_ends(values, key, least, high):
    index_at = [jax.random.randint(jax.random.fold_in(key, axis), (), 0, length) for axis, length in enumerate(values.shape)]
    longest = values.shape.index(max(values.shape))
    neighbour = index_at[:longest] + [(index_at[longest] + 1) % values.shape[longest]] + index_at[longest + 1:]
    return values.at[tuple(index_at)].set(least).at[tuple(neighbour)].set(high)


def levels(key, shape, split, least, top_value):
    factor_of, own = 1.0, jax.random.fold_in(key, 6)
    for axis_at, parts in split:
        steps = jnp.exp(jax.random.uniform(jax.random.fold_in(own, axis_at), (parts,), jnp.float32, least / len(split), top_value / len(split)))
        factor_of = factor_of * jnp.repeat(steps, shape[axis_at] // parts).reshape([-1 if axis == axis_at else 1 for axis in range(len(shape))])
    return factor_of


def bell_draw(rng, dims, scale, limit, cuts=(), kind=jnp.bfloat16):
    gain = levels(rng, dims, cuts, -0.22, 0.18) if cuts else 1.0
    result = jax.random.normal(rng, dims, jnp.float32) * scale * gain
    return jnp.minimum(jnp.maximum(result, -limit), limit).astype(kind)


def setup_inputs(seed: int = 0) -> dict:
    splits = jax.random.split(jax.random.key(seed), 8)
    queries = draw_queries(jax.random.fold_in(splits[7], 71), 0)
    keys = draw_keys(jax.random.fold_in(splits[7], 71), 0)
    values = bell_draw(splits[2], (TOKENS, HEADS * HEAD_DIM), 1.0, 6.0, ((0, 128), (1, 2)))
    grad_out = bell_draw(splits[3], (TOKENS, HEADS * HEAD_DIM), 1.0, 6.0, ((0, 128), (1, 2)))
    bias_table = bell_draw(splits[4], (HEADS, BUCKETS), 1.0, 5.0, ((0, 2),), jnp.float32)
    bucket_ids = set_ends(jax.random.randint(splits[5], (BLOCKS, SPAN, 2 * TOK_DEV), 0, BUCKETS), jax.random.fold_in(splits[5], 1), 0, BUCKETS - 1).astype(jnp.int32)
    block_mask = set_ends((jax.random.randint(splits[6], (BLOCKS, SPAN), 0, 4) < 3).astype(jnp.int32), jax.random.fold_in(splits[6], 1), 0, 1)
    return {"queries": queries, "keys": keys, "values": values, "grad_out": grad_out, "bias_table": bias_table, "bucket_ids": bucket_ids, "block_mask": block_mask}


def reference(queries, keys, values, grad_out, bias_table, bucket_ids, block_mask):
    tok = TOK_DEV
    width = HEADS * HEAD_DIM
    scale = HEAD_DIM ** -0.5
    margin = (SPAN - 1) * tok
    keys_pad = jnp.concatenate([jnp.zeros((margin, width), keys.dtype), keys], axis=0)
    values_pad = jnp.concatenate([jnp.zeros((margin, width), values.dtype), values], axis=0)
    rows = jnp.arange(tok, dtype=jnp.int32)
    window = jnp.arange(SPAN * tok, dtype=jnp.int32)
    offset = SPAN - 1 - window // tok
    inner = window % tok
    position = rows[:, None] - inner[None, :] + tok - 1
    highest = lax.Precision.HIGHEST

    def step(carry, block):
        key_acc, value_acc, bias_acc = carry
        start = (block * tok).astype(jnp.int32)
        query_blk = lax.dynamic_slice_in_dim(queries, start, tok, 0).astype(jnp.float32).reshape(tok, HEADS, HEAD_DIM)
        cot_blk = lax.dynamic_slice_in_dim(grad_out, start, tok, 0).astype(jnp.float32).reshape(tok, HEADS, HEAD_DIM)
        key_win = lax.dynamic_slice_in_dim(keys_pad, start, SPAN * tok, 0).astype(jnp.float32).reshape(SPAN * tok, HEADS, HEAD_DIM)
        value_win = lax.dynamic_slice_in_dim(values_pad, start, SPAN * tok, 0).astype(jnp.float32).reshape(SPAN * tok, HEADS, HEAD_DIM)
        table = lax.dynamic_index_in_dim(bucket_ids, block, 0, keepdims=False)
        ids = table[offset[None, :], position]
        bias = bias_table[:, ids]
        scores = scale * jnp.einsum("qhd,khd->hqk", query_blk, key_win, precision=highest) + bias
        flag_row = lax.dynamic_index_in_dim(block_mask, block, 0, keepdims=False)
        whole = (flag_row[offset] == 1) & (block - offset >= 0)
        valid = jnp.where(offset[None, :] == 0, rows[:, None] >= inner[None, :], whole[None, :])
        masked = jnp.where(valid[None], scores, jnp.float32(-1e30))
        top = masked.max(axis=-1, keepdims=True)
        weights = jnp.where(valid[None], jnp.exp(masked - top), jnp.float32(0.0))
        lse = top[..., 0] + jnp.log(weights.sum(axis=-1))
        prob = jnp.exp(masked - lse[..., None])
        dprob = jnp.einsum("qhd,khd->hqk", cot_blk, value_win, precision=highest)
        delta = (prob * dprob).sum(axis=-1)
        dscore = prob * (dprob - delta[..., None])
        score16 = lax.optimization_barrier(dscore.astype(jnp.bfloat16)).astype(jnp.float32)
        prob16 = lax.optimization_barrier(prob.astype(jnp.bfloat16)).astype(jnp.float32)
        grad_q = scale * jnp.einsum("hqk,khd->qhd", score16, key_win, precision=highest)
        grad_k = scale * jnp.einsum("hqk,qhd->khd", score16, query_blk, precision=highest).reshape(SPAN * tok, width)
        grad_v = jnp.einsum("hqk,qhd->khd", prob16, cot_blk, precision=highest).reshape(SPAN * tok, width)
        key_acc = lax.dynamic_update_slice_in_dim(key_acc, lax.dynamic_slice_in_dim(key_acc, start, SPAN * tok, 0) + grad_k, start, 0)
        value_acc = lax.dynamic_update_slice_in_dim(value_acc, lax.dynamic_slice_in_dim(value_acc, start, SPAN * tok, 0) + grad_v, start, 0)
        bias_acc = bias_acc.at[:, ids].add(dscore)
        return (key_acc, value_acc, bias_acc), grad_q.reshape(tok, width).astype(jnp.bfloat16)

    start_carry = (jnp.zeros((margin + TOKENS, width), jnp.float32), jnp.zeros((margin + TOKENS, width), jnp.float32), jnp.zeros((HEADS, BUCKETS), jnp.float32))
    (key_acc, value_acc, bias_acc), grad_blocks = lax.scan(step, start_carry, jnp.arange(N_SEQ, dtype=jnp.int32))
    grad_queries = grad_blocks.reshape(TOKENS, width)
    grad_keys = key_acc[margin:].astype(jnp.bfloat16)
    grad_values = value_acc[margin:].astype(jnp.bfloat16)
    return grad_queries, grad_keys, grad_values, bias_acc
```

```python
import functools

import jax
import jax.numpy as jnp
from jax import lax
from jax.experimental import pallas as pl
from jax.experimental.pallas import tpu as pltpu
from jax.sharding import PartitionSpec as P

MESH = pl.DeviceIdType.MESH
LOG2E = 1.4426950408889634
NEG = -1e30
F32 = jnp.float32
BF16 = jnp.bfloat16
AHEAD = 3
NT = (((1,), (1,)), ((), ()))


def dot_nt(a, b, **kw):
    return lax.dot_general(a, b, NT, preferred_element_type=F32, **kw)


def dot_nn(a, b, **kw):
    return jnp.dot(a, b, preferred_element_type=F32, **kw)


def kernel(
    sizes,
    q_hbm, k_hbm, v_hbm, do_hbm, table_hbm, ids_hbm, mask_hbm,
    dq_ref, dk_ref, dv_ref, gb_ref,
    kv, qd, tableb, idsb, maskb, byb, biasq, biask,
    ss, sp, dsb, pb, ks, kp, kpb, kdsb, dk0b, dv0b, st, dgb,
    xpart, xbuf, ybuf, zbuf,
    load_sem, small_sem, kv_send, kv_recv, qd_send, qd_recv,
    st_send, st_recv, id_send, id_recv,
    xs_sem, xr_sem, ys_sem, yr_sem, zs_sem, zr_sem,
):
    n_seq, nx, ny, nz, n_head, heads, groups = sizes
    T, W = 128, 128
    scale = 0.125
    c = scale * LOG2E
    me = lax.axis_index("seq")
    hi = lax.axis_index("head")
    core = lax.rem(me, 2)
    partner = me + 1 - 2 * core

    def at(offset):
        return lax.rem(me + (offset + n_seq), n_seq)

    row = 2 * nx
    in_row = lax.rem(me, row)
    row_base = me - in_row
    y_at = lax.rem(me // row, ny)
    z_at = me // (row * ny)
    in_plane = lax.rem(me, row * ny)
    halves = heads // 2
    ring_z = n_head * nz * 2
    in_z = (hi * nz + z_at) * 2 + core

    def x_partner(t):
        return row_base + lax.rem(in_row + t, row)

    def y_partner(t):
        return z_at * (row * ny) + lax.rem(y_at + t, ny) * row + in_row

    def z_partner(t):
        w = lax.rem(in_z + t, ring_z)
        w_core = lax.rem(w, 2)
        w_z = lax.rem(w // 2, nz)
        w_head = w // (2 * nz)
        return {"seq": w_z * (row * ny) + in_plane - core + w_core, "head": w_head}

    srcs = ((q_hbm, qd, 0), (do_hbm, qd, W), (k_hbm, kv, 0), (v_hbm, kv, W))

    def load(n, g):
        src, dst, off = srcs[n]
        return pltpu.make_async_copy(
            src.at[:, pl.ds(g * W, W)], dst.at[g, pl.ds(0, T), pl.ds(off, W)], load_sem.at[n, g]
        )

    for g in range(groups):
        for n in (2, 3, 0, 1):
            load(n, g).start()
    small = [
        pltpu.make_async_copy(table_hbm, tableb, small_sem.at[0]),
        pltpu.make_async_copy(ids_hbm.at[0], idsb.at[0], small_sem.at[1]),
        pltpu.make_async_copy(mask_hbm, maskb.at[0], small_sem.at[2]),
    ]
    for copy in small:
        copy.start()

    barrier = pltpu.get_barrier_semaphore()
    partners = [{"seq": at(o)} for o in (1, 2, 3, -1, -2, -3)]
    partners += [{"seq": x_partner(t)} for t in range(1, row)]
    partners += [{"seq": y_partner(t)} for t in range(1, ny)]
    partners += [z_partner(t) for t in range(1, ring_z)]
    for other in partners:
        pl.semaphore_signal(barrier, inc=1, device_id=other, device_id_type=MESH)

    def remote(src, dst, send, recv, device):
        return pltpu.make_async_remote_copy(
            src_ref=src, dst_ref=dst, send_sem=send, recv_sem=recv, device_id=device, device_id_type=MESH
        )

    def slot(buf, g, s):
        return buf.at[g, pl.ds(s * T, T)]

    def kv_copy(n, g):
        if n == 0:
            src, s, device = slot(kv, g, 0), 2, at(2)
        elif n == 1:
            src, s, device = slot(kv, g, 2), 3, at(1)
        else:
            src, s, device = slot(kv, g, pl.multiple_of(2 * core, 2)), 1, partner
        return remote(src, slot(kv, g, s), kv_send.at[n, g], kv_recv.at[s - 1, g], {"seq": device})

    def qd_copy(n, g):
        if n == 0:
            src, s, device = slot(qd, g, 0), 2, at(-2)
        elif n == 1:
            src, s, device = slot(qd, g, 2), 3, at(-1)
        else:
            src, s, device = slot(qd, g, pl.multiple_of(2 - 2 * core, 2)), 1, partner
        return remote(src, slot(qd, g, s), qd_send.at[n, g], qd_recv.at[s - 1, g], {"seq": device})

    by_slot = {1: 2, 2: 0, 3: 1}

    def kv_arrived(s, g):
        kv_copy(by_slot[s], g).wait_recv()

    def qd_arrived(s, g):
        qd_copy(by_slot[s], g).wait_recv()

    def st_copy(s, g):
        return remote(st.at[0, g], st.at[s, g], st_send.at[s - 1, g], st_recv.at[s - 1, g], {"seq": at(-s)})

    def id_copy(s):
        return remote(idsb.at[0], idsb.at[s], id_send.at[0, s - 1], id_recv.at[0, s - 1], {"seq": at(-s)})

    def mask_copy(s):
        return remote(maskb.at[0], maskb.at[s], id_send.at[1, s - 1], id_recv.at[1, s - 1], {"seq": at(-s)})

    def send_own(g):
        kv_copy(0, g).start()
        qd_copy(0, g).start()

    for copy in small:
        copy.wait()
    for g in range(groups):
        for n in (2, 3, 0, 1):
            load(n, g).wait()
    pl.semaphore_wait(barrier, len(partners))
    for g in range(AHEAD):
        send_own(g)
    for s in (1, 2, 3):
        id_copy(s).start()
        mask_copy(s).start()

    lane = lax.broadcasted_iota(jnp.int32, (T, T), 1)
    first = lane < 64
    lane8 = lax.broadcasted_iota(jnp.int32, (8, T), 1)
    sub8 = lax.broadcasted_iota(jnp.int32, (8, T), 0)
    codes = lax.broadcasted_iota(jnp.int32, (T, 2 * T), 0)

    def onehot(place, s):
        return (codes == idsb[place, s : s + 1, :]).astype(F32)

    def by_offset(place, s, inside):
        by = dot_nn(tableb[...] * LOG2E, onehot(place, s), precision=lax.Precision.HIGHEST)
        if s:
            keep = jnp.logical_and(maskb[place, 0:1, s : s + 1] == 1, inside)
            by = jnp.where(keep, by, NEG)
        return pltpu.roll(by, 1, 1)

    def skewed(index, head):
        line = jnp.broadcast_to(byb[index, pl.ds(head, 1), :], (8, 2 * T))
        base = pltpu.roll(line, 0, 1, stride=1, stride_axis=0)
        return base[:, :T], base[:, T:]

    def block_row(low, high, a):
        mixed = jnp.where(lane8 >= T - 8 * a, low, high)
        return pltpu.roll(mixed, 8 * a, 1) if a else mixed

    for s in range(4):
        byb[s] = by_offset(0, s, me >= s)

    def build_query(g, carry):
        for h in range(2):
            for s in range(4):
                low, high = skewed(s, 2 * g + h)
                for a in range(16):
                    x = block_row(low, high, a)
                    if s == 0:
                        x = jnp.where(8 * a + sub8 <= lane8, x, NEG)
                    biasq[g, pl.ds(s * T + 8 * a, 8), pl.ds(h * T, T)] = x
        return carry

    lax.fori_loop(0, groups, build_query, 0)
    for s in (1, 2, 3):
        id_copy(s).wait_recv()
        mask_copy(s).wait_recv()
        byb[3 + s] = by_offset(s, s, me + s < n_seq)

    def build_key(g, carry):
        for h in range(2):
            for s in (1, 2, 3):
                low, high = skewed(3 + s, 2 * g + h)
                for a in range(16):
                    biask[g, pl.ds(h * T + 8 * a, 8), pl.ds((s - 1) * T, T)] = block_row(low, high, a)
        return carry

    lax.fori_loop(0, groups, build_key, 0)

    def two(x):
        zero = jnp.zeros_like(x)
        return jnp.concatenate([jnp.where(first, x, zero), jnp.where(first, zero, x)], axis=0)

    def merged(x):
        return jnp.where(first, x[:T], x[T:])

    R = 32

    def fold(x, op):
        parts = [x[8 * j : 8 * j + 8] for j in range(x.shape[0] // 8)]
        return functools.reduce(op, parts)

    def query_side(g):
        q2, do2 = qd[g, 0:T, 0:W], qd[g, 0:T, W : 2 * W]
        ss[...] = dot_nt(kv[g, :, 0:W], two(q2))
        sp[...] = dot_nt(kv[g, :, W : 2 * W], two(do2))
        top = jnp.full((8, 2 * T), NEG, F32)
        for r in range(0, 4 * T, R):
            x = ss[r : r + R] * c + biasq[g, r : r + R]
            ss[r : r + R] = x
            top = jnp.maximum(top, fold(x, jnp.maximum))
        top = top.max(axis=0, keepdims=True)
        total = jnp.zeros((8, 2 * T), F32)
        accum = jnp.zeros((8, 2 * T), F32)
        for r in range(0, 4 * T, R):
            e = jnp.exp2(ss[r : r + R] - top)
            ss[r : r + R] = e
            total = total + fold(e, jnp.add)
            accum = accum + fold(e * sp[r : r + R], jnp.add)
        total = total.sum(axis=0, keepdims=True)
        accum = accum.sum(axis=0, keepdims=True)
        inverse = 1.0 / total
        delta = accum / total
        lse = top + jnp.log2(total)
        st[0, g, 0:1, :] = lse[:, :T]
        st[0, g, 1:2, :] = lse[:, T:]
        st[0, g, 2:3, :] = delta[:, :T]
        st[0, g, 3:4, :] = delta[:, T:]
        for s in range(4):
            low = [jnp.zeros((8, T), F32) for _ in range(2)]
            high = [jnp.zeros((8, T), F32) for _ in range(2)]
            for r in range(s * T, s * T + T, R):
                p = ss[r : r + R] * inverse
                ds = p * (sp[r : r + R] - delta)
                dsb[r : r + R] = ds.astype(BF16)
                if s == 0:
                    pb[r : r + R] = p.astype(BF16)
                for j in range(R // 8):
                    a = (r - s * T) // 8 + j
                    for h in range(2):
                        x = ds[8 * j : 8 * j + 8, h * T : h * T + T]
                        if a:
                            x = pltpu.roll(x, T - 8 * a, 1)
                            here = lane8 < T - 8 * a
                            high[h] = high[h] + jnp.where(here, x, 0.0)
                            low[h] = low[h] + jnp.where(here, 0.0, x)
                        else:
                            high[h] = high[h] + x
            for h in range(2):
                both = jnp.concatenate([low[h], high[h]], axis=1)
                for by in (1, 2, 4):
                    both = both + pltpu.roll(pltpu.roll(both, 2 * T - by, 1), 8 - by, 0)
                dgb[s, pl.ds(2 * g + h, 1), :] = both[0:1]
        turned = dot_nn(kv[g, :, 0:W].T, dsb[...])
        joined = jnp.concatenate([turned[0:64, 0:T], turned[64:T, T : 2 * T]], axis=0)
        dq_ref[:, pl.ds(g * W, W)] = (joined.T * scale).astype(BF16)
        for s in (1, 2, 3):
            st_copy(s, g).start()
        dv0b[g] = jnp.where(first, dot_nn(pb[:, 0:T], do2), dot_nn(pb[:, T : 2 * T], do2))
        dk0b[g] = jnp.where(first, dot_nn(dsb[0:T, 0:T], q2), dot_nn(dsb[0:T, T : 2 * T], q2))

    def key_side(g):
        qs, dos = qd[g, T : 4 * T, 0:W], qd[g, T : 4 * T, W : 2 * W]
        ks[...] = dot_nt(two(kv[g, 0:T, 0:W]), qs)
        kp[...] = dot_nt(two(kv[g, 0:T, W : 2 * W]), dos)
        for h in range(2):
            for s in (1, 2, 3):
                lse = st[s, g, h : h + 1, :]
                delta = st[s, g, 2 + h : 3 + h, :]
                cols = slice((s - 1) * T, s * T)
                for r in range(h * T, h * T + T, R):
                    x = ks[r : r + R, cols] * c + biask[g, r : r + R, cols]
                    p = jnp.exp2(x - lse)
                    ds = p * (kp[r : r + R, cols] - delta)
                    kpb[r : r + R, cols] = p.astype(BF16)
                    kdsb[r : r + R, cols] = ds.astype(BF16)
        dv_ref[:, pl.ds(g * W, W)] = (merged(dot_nn(kpb[...], dos)) + dv0b[g]).astype(BF16)
        dk_ref[:, pl.ds(g * W, W)] = ((merged(dot_nn(kdsb[...], qs)) + dk0b[g]) * scale).astype(BF16)

    def key_ready(g):
        for s in (1, 3):
            qd_arrived(s, g)
        for s in (1, 2, 3):
            st_copy(s, g).wait_recv()

    def step(g, carry):
        kv_arrived(2, g)
        kv_copy(1, g).start()
        kv_copy(2, g).start()
        qd_arrived(2, g)
        qd_copy(1, g).start()
        qd_copy(2, g).start()

        @pl.when(g + AHEAD < groups)
        def _():
            send_own(g + AHEAD)

        kv_arrived(3, g)
        kv_arrived(1, g)
        query_side(g)

        @pl.when(g > 0)
        def _():
            key_ready(g - 1)
            key_side(g - 1)

        return carry

    lax.fori_loop(0, groups, step, 0)

    part = jnp.zeros((heads, T), F32)
    for s in range(4):
        part = part + dot_nt(pltpu.roll(dgb[s], 2 * T - 1, 1), onehot(0, s), precision=lax.Precision.HIGHEST)
    xpart[...] = part

    def x_copy(t):
        other = x_partner(t)
        half = pl.multiple_of(lax.rem(other, 2) * halves, halves)
        return remote(xpart.at[pl.ds(half, halves)], xbuf.at[in_row], xs_sem.at[t - 1], xr_sem.at[t - 1], {"seq": other})

    def y_copy(t):
        return remote(ybuf.at[y_at], ybuf.at[y_at], ys_sem.at[t - 1], yr_sem.at[t - 1], {"seq": y_partner(t)})

    def z_copy(t):
        return remote(zbuf.at[in_z], zbuf.at[in_z], zs_sem.at[t - 1], zr_sem.at[t - 1], z_partner(t))

    def total_of(buf, slots):
        return functools.reduce(jnp.add, [buf[i] for i in slots])

    for t in range(1, row):
        x_copy(t).start()
    xbuf[in_row] = xpart[pl.ds(pl.multiple_of(core * halves, halves), halves), :]
    key_ready(groups - 1)
    key_side(groups - 1)
    for t in range(1, row):
        x_copy(t).wait_recv()
    ybuf[y_at] = total_of(xbuf, range(row))
    for t in range(1, ny):
        y_copy(t).start()
    for t in range(1, ny):
        y_copy(t).wait_recv()
    zbuf[in_z] = total_of(ybuf, range(ny))
    for t in range(1, ring_z):
        z_copy(t).start()
    for t in range(1, ring_z):
        z_copy(t).wait_recv()
    for h in range(n_head):
        for half in range(2):
            gb_ref[h * heads + half * halves : h * heads + (half + 1) * halves] = total_of(
                zbuf, [(h * nz + z) * 2 + half for z in range(nz)]
            )

    def drain(g, carry):
        for n in range(3):
            kv_copy(n, g).wait_send()
            qd_copy(n, g).wait_send()
        for s in (1, 2, 3):
            st_copy(s, g).wait_send()
        return carry

    lax.fori_loop(0, groups, drain, 0)
    for s in (1, 2, 3):
        id_copy(s).wait_send()
        mask_copy(s).wait_send()
    for t in range(1, row):
        x_copy(t).wait_send()
    for t in range(1, ny):
        y_copy(t).wait_send()
    for t in range(1, ring_z):
        z_copy(t).wait_send()


def solution(mesh):
    n_seq, n_head = mesh.shape["seq"], mesh.shape["head"]
    nx, ny, nz = (4, 4, 4) if n_seq == 128 else (2, 1, 2)

    def body(queries, keys, values, grad_out, bias_table, bucket_ids, block_mask):
        tok, width = queries.shape
        heads, buckets = bias_table.shape
        groups = width // 128
        sizes = (n_seq, nx, ny, nz, n_head, heads, groups)
        row = 2 * nx
        ring_z = n_head * nz * 2
        operands = (queries, keys, values, grad_out, bias_table, bucket_ids, block_mask)
        V = pltpu.VMEM
        dma = pltpu.SemaphoreType.DMA
        scratch = [
            V((groups, 512, 256), BF16), V((groups, 512, 256), BF16),
            V((heads, 128), F32), V((4, 4, 256), jnp.int32), V((4, 1, 4), jnp.int32),
            V((7, heads, 256), F32), V((groups, 512, 256), F32), V((groups, 256, 384), F32),
            V((512, 256), F32), V((512, 256), F32), V((512, 256), BF16), V((128, 256), BF16),
            V((256, 384), F32), V((256, 384), F32), V((256, 384), BF16), V((256, 384), BF16),
            V((groups, 128, 128), F32), V((groups, 128, 128), F32),
            V((4, groups, 8, 128), F32), V((4, heads, 256), F32),
            V((heads, 128), F32), V((row, heads // 2, 128), F32), V((ny, heads // 2, 128), F32),
            V((ring_z, heads // 2, 128), F32),
            dma((4, groups)), dma((3,)),
            dma((3, groups)), dma((3, groups)), dma((3, groups)), dma((3, groups)),
            dma((3, groups)), dma((3, groups)), dma((2, 3)), dma((2, 3)),
            dma((row - 1,)), dma((row - 1,)), dma((max(ny - 1, 1),)), dma((max(ny - 1, 1),)),
            dma((ring_z - 1,)), dma((ring_z - 1,)),
        ]
        in_hbm = pl.BlockSpec(memory_space=pltpu.HBM)
        in_vmem = pl.BlockSpec(memory_space=pltpu.VMEM)
        out = jax.ShapeDtypeStruct((tok, width), BF16)
        return pl.pallas_call(
            functools.partial(kernel, sizes),
            out_shape=(out, out, out, jax.ShapeDtypeStruct((n_head * heads, buckets), F32)),
            in_specs=[in_hbm] * 7,
            out_specs=(in_vmem,) * 4,
            scratch_shapes=scratch,
            compiler_params=pltpu.CompilerParams(
                collective_id=0, has_side_effects=True, vmem_limit_bytes=48 * 1024 * 1024
            ),
        )(*(pltpu.with_memory_space_constraint(x, pltpu.HBM) for x in operands))

    block = P("seq", "head")
    return jax.shard_map(
        body,
        mesh=mesh,
        in_specs=(block, block, block, block, P("head", None), P("seq", None, None), P("seq", None)),
        out_specs=(block, block, block, P(None, None)),
        check_vma=False,
    )
```

```python
import functools

import jax
import jax.numpy as jnp
from jax import lax
from jax.experimental import pallas as pl
from jax.experimental.pallas import tpu as pltpu
from jax.sharding import PartitionSpec as P

MESH = pl.DeviceIdType.MESH
LOG2E = 1.4426950408889634
NEG = -1e30
F32 = jnp.float32
BF16 = jnp.bfloat16
AHEAD = 5
RELAY = 2
LAG = 4
NT = (((1,), (1,)), ((), ()))


def dot_nt(a, b, **kw):
    return lax.dot_general(a, b, NT, preferred_element_type=F32, **kw)


def dot_nn(a, b, **kw):
    return jnp.dot(a, b, preferred_element_type=F32, **kw)


def kernel(
    sizes,
    q_hbm, k_hbm, v_hbm, do_hbm, table_hbm, ids_hbm, mask_hbm,
    dq_ref, dk_ref, dv_ref, gb_ref,
    kv, qd, tableb, idsb, maskb, byb, biasq, biask,
    ss, sp, dsb, pb, ks, kp, kpb, kdsb, dk0b, dv0b, st, dgb,
    xpart, xbuf, ybuf, zbuf,
    load_sem, small_sem, kv_send, kv_recv, qd_send, qd_recv,
    st_send, st_recv, id_send, id_recv,
    xs_sem, xr_sem, ys_sem, yr_sem, zs_sem, zr_sem,
):
    n_seq, nx, ny, nz, n_head, heads, groups = sizes
    T, W = 128, 128
    scale = 0.125
    c = scale * LOG2E
    me = lax.axis_index("seq")
    hi = lax.axis_index("head")
    core = lax.rem(me, 2)
    partner = me + 1 - 2 * core

    def at(offset):
        return lax.rem(me + (offset + n_seq), n_seq)

    row = 2 * nx
    in_row = lax.rem(me, row)
    row_base = me - in_row
    y_at = lax.rem(me // row, ny)
    z_at = me // (row * ny)
    in_plane = lax.rem(me, row * ny)
    halves = heads // 2
    ring_z = n_head * nz * 2
    in_z = (hi * nz + z_at) * 2 + core

    def x_partner(t):
        return row_base + lax.rem(in_row + t, row)

    def y_partner(t):
        return z_at * (row * ny) + lax.rem(y_at + t, ny) * row + in_row

    def z_partner(t):
        w = lax.rem(in_z + t, ring_z)
        w_core = lax.rem(w, 2)
        w_z = lax.rem(w // 2, nz)
        w_head = w // (2 * nz)
        return {"seq": w_z * (row * ny) + in_plane - core + w_core, "head": w_head}

    srcs = ((q_hbm, qd, 0), (do_hbm, qd, W), (k_hbm, kv, 0), (v_hbm, kv, W))

    def load(n, g):
        src, dst, off = srcs[n]
        return pltpu.make_async_copy(
            src.at[:, pl.ds(g * W, W)], dst.at[g, pl.ds(0, T), pl.ds(off, W)], load_sem.at[n, g]
        )

    for g in range(groups):
        for n in (2, 3, 0, 1):
            load(n, g).start()
    small = [
        pltpu.make_async_copy(table_hbm, tableb, small_sem.at[0]),
        pltpu.make_async_copy(ids_hbm.at[0], idsb.at[0], small_sem.at[1]),
        pltpu.make_async_copy(mask_hbm, maskb.at[0], small_sem.at[2]),
    ]
    for copy in small:
        copy.start()

    barrier = pltpu.get_barrier_semaphore()
    partners = [{"seq": at(o)} for o in (1, 2, 3, -1, -2, -3)]
    partners += [{"seq": x_partner(t)} for t in range(1, row)]
    partners += [{"seq": y_partner(t)} for t in range(1, ny)]
    partners += [z_partner(t) for t in range(1, ring_z)]
    for other in partners:
        pl.semaphore_signal(barrier, inc=1, device_id=other, device_id_type=MESH)

    def remote(src, dst, send, recv, device):
        return pltpu.make_async_remote_copy(
            src_ref=src, dst_ref=dst, send_sem=send, recv_sem=recv, device_id=device, device_id_type=MESH
        )

    def slot(buf, g, s):
        return buf.at[g, pl.ds(s * T, T)]

    def kv_copy(n, g):
        if n == 0:
            src, s, device = slot(kv, g, 0), 2, at(2)
        elif n == 1:
            src, s, device = slot(kv, g, 2), 3, at(1)
        else:
            src, s, device = slot(kv, g, pl.multiple_of(2 * core, 2)), 1, partner
        return remote(src, slot(kv, g, s), kv_send.at[n, g], kv_recv.at[s - 1, g], {"seq": device})

    def qd_copy(n, g):
        if n == 0:
            src, s, device = slot(qd, g, 0), 2, at(-2)
        elif n == 1:
            src, s, device = slot(qd, g, 2), 3, at(-1)
        else:
            src, s, device = slot(qd, g, pl.multiple_of(2 - 2 * core, 2)), 1, partner
        return remote(src, slot(qd, g, s), qd_send.at[n, g], qd_recv.at[s - 1, g], {"seq": device})

    after = n_seq - 1 - me
    kv_sent = (after >= 2, jnp.logical_and(me >= 2, after >= 1), jnp.logical_or(core == 0, me >= 2))
    qd_sent = (me >= 2, jnp.logical_and(after >= 2, me >= 1), jnp.logical_or(core == 1, after >= 2))
    by_slot = {1: 2, 2: 0, 3: 1}

    def kv_start(n, g):
        pl.when(kv_sent[n])(lambda: kv_copy(n, g).start())

    def qd_start(n, g):
        pl.when(qd_sent[n])(lambda: qd_copy(n, g).start())

    def kv_arrived(s, g):
        pl.when(me >= s)(lambda: kv_copy(by_slot[s], g).wait_recv())

    def qd_arrived(s, g):
        pl.when(after >= s)(lambda: qd_copy(by_slot[s], g).wait_recv())

    def st_copy(s, g):
        return remote(st.at[0, g], st.at[s, g], st_send.at[s - 1, g], st_recv.at[s - 1, g], {"seq": at(-s)})

    def id_copy(s):
        return remote(idsb.at[0], idsb.at[s], id_send.at[0, s - 1], id_recv.at[0, s - 1], {"seq": at(-s)})

    def mask_copy(s):
        return remote(maskb.at[0], maskb.at[s], id_send.at[1, s - 1], id_recv.at[1, s - 1], {"seq": at(-s)})

    def send_own(g):
        kv_start(0, g)
        qd_start(0, g)

    def kv_relay(g):
        kv_arrived(2, g)
        kv_start(1, g)
        kv_start(2, g)

    def qd_relay(g):
        qd_arrived(2, g)
        qd_start(1, g)
        qd_start(2, g)

    with jax.named_scope("load_wait"):
        for copy in small:
            copy.wait()
        for g in range(groups):
            for n in (2, 3, 0, 1):
                load(n, g).wait()
    with jax.named_scope("barrier"):
        pl.semaphore_wait(barrier, len(partners))
    for s in (1, 2, 3):

        @pl.when(me >= s)
        def _():
            id_copy(s).start()
            mask_copy(s).start()

    for g in range(AHEAD):
        send_own(g)
    for s in (1, 2, 3):

        @pl.when(me < s)
        def _():
            kv[:, pl.ds(s * T, T), :] = jnp.zeros((groups, T, 2 * W), BF16)

        @pl.when(after < s)
        def _():
            qd[:, pl.ds(s * T, T), :] = jnp.zeros((groups, T, 2 * W), BF16)
            st[s] = jnp.zeros((groups, 8, T), F32)
            idsb[s] = jnp.zeros((4, 2 * T), jnp.int32)
            maskb[s] = jnp.zeros((1, 4), jnp.int32)

    lane = lax.broadcasted_iota(jnp.int32, (T, T), 1)
    first = lane < 64
    lane8 = lax.broadcasted_iota(jnp.int32, (8, T), 1)
    sub8 = lax.broadcasted_iota(jnp.int32, (8, T), 0)
    codes = lax.broadcasted_iota(jnp.int32, (T, 2 * T), 0)

    def onehot(place, s):
        return (codes == idsb[place, s : s + 1, :]).astype(BF16)

    def thirds(x):
        big = x.astype(BF16)
        rest = x - big.astype(F32)
        mid = rest.astype(BF16)
        return jnp.concatenate([big, mid, (rest - mid.astype(F32)).astype(BF16)], axis=0)

    def whole(x):
        n = x.shape[0] // 3
        return x[:n] + x[n : 2 * n] + x[2 * n :]

    def by_offset(place, s, inside):
        by = whole(dot_nn(thirds(tableb[...] * LOG2E), onehot(place, s)))
        if s:
            keep = jnp.logical_and(maskb[place, 0:1, s : s + 1] == 1, inside)
            by = jnp.where(keep, by, NEG)
        return pltpu.roll(by, 1, 1)

    def skewed(index, head):
        line = jnp.broadcast_to(byb[index, pl.ds(head, 1), :], (8, 2 * T))
        base = pltpu.roll(line, 0, 1, stride=1, stride_axis=0)
        return base[:, :T], base[:, T:]

    def block_row(low, high, a):
        mixed = jnp.where(lane8 >= T - 8 * a, low, high)
        return pltpu.roll(mixed, 8 * a, 1) if a else mixed

    with jax.named_scope("by"):
        for s in range(4):
            byb[s] = by_offset(0, s, me >= s)

    def build_query(g, carry):
        for h in range(2):
            for s in range(4):
                low, high = skewed(s, 2 * g + h)
                for a in range(16):
                    x = block_row(low, high, a)
                    if s == 0:
                        x = jnp.where(8 * a + sub8 <= lane8, x, NEG)
                    biasq[g, pl.ds(s * T + 8 * a, 8), pl.ds(h * T, T)] = x
        return carry

    with jax.named_scope("build_query"):
        lax.fori_loop(0, groups, build_query, 0)
    with jax.named_scope("relay_first"):
        kv_relay(0)
    with jax.named_scope("by_key"):
        for s in (1, 2, 3):

            @pl.when(after >= s)
            def _():
                id_copy(s).wait_recv()
                mask_copy(s).wait_recv()

            byb[3 + s] = by_offset(s, s, after >= s)

    def build_key(g, carry):
        for h in range(2):
            for s in (1, 2, 3):
                low, high = skewed(3 + s, 2 * g + h)
                for a in range(16):
                    biask[g, pl.ds(h * T + 8 * a, 8), pl.ds((s - 1) * T, T)] = block_row(low, high, a)
        return carry

    with jax.named_scope("build_key"):
        lax.fori_loop(0, groups, build_key, 0)
    with jax.named_scope("relay_first"):
        for g in range(1, RELAY):
            kv_relay(g)

    def two(x):
        zero = jnp.zeros_like(x)
        return jnp.concatenate([jnp.where(first, x, zero), jnp.where(first, zero, x)], axis=0)

    def merged(x):
        return jnp.where(first, x[:T], x[T:])

    R = 32

    def fold(x, op):
        parts = [x[8 * j : 8 * j + 8] for j in range(x.shape[0] // 8)]
        return functools.reduce(op, parts)

    def query_side(g):
        q2, do2 = qd[g, 0:T, 0:W], qd[g, 0:T, W : 2 * W]
        ss[...] = dot_nt(kv[g, :, 0:W], two(q2))
        sp[...] = dot_nt(kv[g, :, W : 2 * W], two(do2))
        top = jnp.full((8, 2 * T), NEG, F32)
        for r in range(0, 4 * T, R):
            x = ss[r : r + R] * c + biasq[g, r : r + R]
            ss[r : r + R] = x
            top = jnp.maximum(top, fold(x, jnp.maximum))
        top = top.max(axis=0, keepdims=True)
        total = jnp.zeros((8, 2 * T), F32)
        accum = jnp.zeros((8, 2 * T), F32)
        for r in range(0, 4 * T, R):
            e = jnp.exp2(ss[r : r + R] - top)
            ss[r : r + R] = e
            total = total + fold(e, jnp.add)
            accum = accum + fold(e * sp[r : r + R], jnp.add)
        total = total.sum(axis=0, keepdims=True)
        accum = accum.sum(axis=0, keepdims=True)
        inverse = 1.0 / total
        delta = accum / total
        lse = top + jnp.log2(total)
        st[0, g, 0:1, :] = lse[:, :T]
        st[0, g, 1:2, :] = lse[:, T:]
        st[0, g, 2:3, :] = delta[:, :T]
        st[0, g, 3:4, :] = delta[:, T:]
        for s in range(4):
            low = [jnp.zeros((8, T), F32) for _ in range(2)]
            high = [jnp.zeros((8, T), F32) for _ in range(2)]
            for r in range(s * T, s * T + T, R):
                p = ss[r : r + R] * inverse
                ds = p * (sp[r : r + R] - delta)
                dsb[r : r + R] = ds.astype(BF16)
                if s == 0:
                    pb[r : r + R] = p.astype(BF16)
                for j in range(R // 8):
                    a = (r - s * T) // 8 + j
                    for h in range(2):
                        x = ds[8 * j : 8 * j + 8, h * T : h * T + T]
                        if a:
                            x = pltpu.roll(x, T - 8 * a, 1)
                            here = lane8 < T - 8 * a
                            high[h] = high[h] + jnp.where(here, x, 0.0)
                            low[h] = low[h] + jnp.where(here, 0.0, x)
                        else:
                            high[h] = high[h] + x
            for h in range(2):
                both = jnp.concatenate([low[h], high[h]], axis=1)
                for by in (1, 2, 4):
                    both = both + pltpu.roll(pltpu.roll(both, 2 * T - by, 1), 8 - by, 0)
                dgb[s, pl.ds(2 * g + h, 1), :] = both[0:1]
        turned = dot_nn(kv[g, :, 0:W].T, dsb[...])
        joined = jnp.concatenate([turned[0:64, 0:T], turned[64:T, T : 2 * T]], axis=0)
        dq_ref[:, pl.ds(g * W, W)] = (joined.T * scale).astype(BF16)
        for s in (1, 2, 3):
            pl.when(me >= s)(lambda s=s: st_copy(s, g).start())
        dv0b[g] = jnp.where(first, dot_nn(pb[:, 0:T], do2), dot_nn(pb[:, T : 2 * T], do2))
        dk0b[g] = jnp.where(first, dot_nn(dsb[0:T, 0:T], q2), dot_nn(dsb[0:T, T : 2 * T], q2))

    def key_side(g):
        qs, dos = qd[g, T : 4 * T, 0:W], qd[g, T : 4 * T, W : 2 * W]
        ks[...] = dot_nt(two(kv[g, 0:T, 0:W]), qs)
        kp[...] = dot_nt(two(kv[g, 0:T, W : 2 * W]), dos)
        for h in range(2):
            for s in (1, 2, 3):
                lse = st[s, g, h : h + 1, :]
                delta = st[s, g, 2 + h : 3 + h, :]
                cols = slice((s - 1) * T, s * T)
                for r in range(h * T, h * T + T, R):
                    x = ks[r : r + R, cols] * c + biask[g, r : r + R, cols]
                    p = jnp.exp2(x - lse)
                    ds = p * (kp[r : r + R, cols] - delta)
                    kpb[r : r + R, cols] = p.astype(BF16)
                    kdsb[r : r + R, cols] = ds.astype(BF16)
        dv_ref[:, pl.ds(g * W, W)] = (merged(dot_nn(kpb[...], dos)) + dv0b[g]).astype(BF16)
        dk_ref[:, pl.ds(g * W, W)] = ((merged(dot_nn(kdsb[...], qs)) + dk0b[g]) * scale).astype(BF16)

    def key_ready(g):
        for s in (1, 3):
            qd_arrived(s, g)
        for s in (1, 2, 3):
            pl.when(after >= s)(lambda s=s: st_copy(s, g).wait_recv())

    def step(g, carry):
        with jax.named_scope("relay"):
            pl.when(g + RELAY < groups)(lambda: kv_relay(g + RELAY))
            pl.when(g + AHEAD < groups)(lambda: send_own(g + AHEAD))
            qd_relay(g)
        with jax.named_scope("kv_wait"):
            kv_arrived(3, g)
            kv_arrived(1, g)
        with jax.named_scope("query"):
            query_side(g)

        @pl.when(g >= LAG)
        def _():
            with jax.named_scope("key_wait"):
                key_ready(g - LAG)
            with jax.named_scope("key"):
                key_side(g - LAG)

        return carry

    lax.fori_loop(0, groups, step, 0)

    part = jnp.zeros((heads, T), F32)
    with jax.named_scope("buckets"):
        for s in range(4):
            part = part + whole(dot_nt(thirds(pltpu.roll(dgb[s], 2 * T - 1, 1)), onehot(0, s)))
    xpart[...] = part

    def x_copy(t):
        other = x_partner(t)
        half = pl.multiple_of(lax.rem(other, 2) * halves, halves)
        return remote(xpart.at[pl.ds(half, halves)], xbuf.at[in_row], xs_sem.at[t - 1], xr_sem.at[t - 1], {"seq": other})

    def y_copy(t):
        return remote(ybuf.at[y_at], ybuf.at[y_at], ys_sem.at[t - 1], yr_sem.at[t - 1], {"seq": y_partner(t)})

    def z_copy(t):
        return remote(zbuf.at[in_z], zbuf.at[in_z], zs_sem.at[t - 1], zr_sem.at[t - 1], z_partner(t))

    def total_of(buf, slots):
        return functools.reduce(jnp.add, [buf[i] for i in slots])

    for t in range(1, row):
        x_copy(t).start()
    xbuf[in_row] = xpart[pl.ds(pl.multiple_of(core * halves, halves), halves), :]
    with jax.named_scope("key"):
        for g in range(groups - 4, groups - 2):
            key_ready(g)
            key_side(g)
    with jax.named_scope("sum_x"):
        for t in range(1, row):
            x_copy(t).wait_recv()
        ybuf[y_at] = total_of(xbuf, range(row))
    for t in range(1, ny):
        y_copy(t).start()
    with jax.named_scope("key"):
        key_ready(groups - 2)
        key_side(groups - 2)
    with jax.named_scope("sum_y"):
        for t in range(1, ny):
            y_copy(t).wait_recv()
        zbuf[in_z] = total_of(ybuf, range(ny))
    for t in range(1, ring_z):
        z_copy(t).start()
    with jax.named_scope("key"):
        key_ready(groups - 1)
        key_side(groups - 1)
    with jax.named_scope("sum_z"):
        for t in range(1, ring_z):
            z_copy(t).wait_recv()
    for h in range(n_head):
        for half in range(2):
            gb_ref[h * heads + half * halves : h * heads + (half + 1) * halves] = total_of(
                zbuf, [(h * nz + z) * 2 + half for z in range(nz)]
            )

    def drain(g, carry):
        for n in range(3):
            pl.when(kv_sent[n])(lambda n=n: kv_copy(n, g).wait_send())
            pl.when(qd_sent[n])(lambda n=n: qd_copy(n, g).wait_send())
        for s in (1, 2, 3):
            pl.when(me >= s)(lambda s=s: st_copy(s, g).wait_send())
        return carry

    with jax.named_scope("drain"):
        lax.fori_loop(0, groups, drain, 0)
    for s in (1, 2, 3):

        @pl.when(me >= s)
        def _():
            id_copy(s).wait_send()
            mask_copy(s).wait_send()

    for t in range(1, row):
        x_copy(t).wait_send()
    for t in range(1, ny):
        y_copy(t).wait_send()
    for t in range(1, ring_z):
        z_copy(t).wait_send()


def put_out(*refs):
    sems = refs[8]
    copies = [pltpu.make_async_copy(refs[i], refs[4 + i], sems.at[i]) for i in range(4)]
    for copy in copies:
        copy.start()
    for copy in copies:
        copy.wait()


def solution(mesh):
    n_seq, n_head = mesh.shape["seq"], mesh.shape["head"]
    nx, ny, nz = (4, 4, 4) if n_seq == 128 else (2, 1, 2)

    def body(queries, keys, values, grad_out, bias_table, bucket_ids, block_mask):
        tok, width = queries.shape
        heads, buckets = bias_table.shape
        groups = width // 128
        sizes = (n_seq, nx, ny, nz, n_head, heads, groups)
        row = 2 * nx
        ring_z = n_head * nz * 2
        operands = (queries, keys, values, grad_out, bias_table, bucket_ids, block_mask)
        V = pltpu.VMEM
        dma = pltpu.SemaphoreType.DMA
        scratch = [
            V((groups, 512, 256), BF16), V((groups, 512, 256), BF16),
            V((heads, 128), F32), V((4, 4, 256), jnp.int32), V((4, 1, 4), jnp.int32),
            V((7, heads, 256), F32), V((groups, 512, 256), F32), V((groups, 256, 384), F32),
            V((512, 256), F32), V((512, 256), F32), V((512, 256), BF16), V((128, 256), BF16),
            V((256, 384), F32), V((256, 384), F32), V((256, 384), BF16), V((256, 384), BF16),
            V((groups, 128, 128), F32), V((groups, 128, 128), F32),
            V((4, groups, 8, 128), F32), V((4, heads, 256), F32),
            V((heads, 128), F32), V((row, heads // 2, 128), F32), V((ny, heads // 2, 128), F32),
            V((ring_z, heads // 2, 128), F32),
            dma((4, groups)), dma((3,)),
            dma((3, groups)), dma((3, groups)), dma((3, groups)), dma((3, groups)),
            dma((3, groups)), dma((3, groups)), dma((2, 3)), dma((2, 3)),
            dma((row - 1,)), dma((row - 1,)), dma((max(ny - 1, 1),)), dma((max(ny - 1, 1),)),
            dma((ring_z - 1,)), dma((ring_z - 1,)),
        ]
        in_hbm = pl.BlockSpec(memory_space=pltpu.HBM)
        in_vmem = pl.BlockSpec(memory_space=pltpu.VMEM)
        out = jax.ShapeDtypeStruct((tok, width), BF16)
        shapes = (out, out, out, jax.ShapeDtypeStruct((n_head * heads, buckets), F32))
        results = pl.pallas_call(
            functools.partial(kernel, sizes),
            out_shape=shapes,
            in_specs=[in_hbm] * 7,
            out_specs=(in_vmem,) * 4,
            scratch_shapes=scratch,
            compiler_params=pltpu.CompilerParams(
                collective_id=0, has_side_effects=True, vmem_limit_bytes=48 * 1024 * 1024
            ),
        )(*(pltpu.with_memory_space_constraint(x, pltpu.HBM) for x in operands))
        return pl.pallas_call(
            put_out,
            out_shape=shapes,
            in_specs=[in_vmem] * 4,
            out_specs=(pl.BlockSpec(memory_space=pltpu.HBM),) * 4,
            scratch_shapes=[dma((4,))],
        )(*(pltpu.with_memory_space_constraint(x, pltpu.VMEM) for x in results))

    block = P("seq", "head")
    return jax.shard_map(
        body,
        mesh=mesh,
        in_specs=(block, block, block, block, P("head", None), P("seq", None, None), P("seq", None)),
        out_specs=(block, block, block, P(None, None)),
        check_vma=False,
    )
```

```python
import functools

import jax
import jax.numpy as jnp
from jax import lax
from jax.experimental import pallas as pl
from jax.experimental.pallas import tpu as pltpu
from jax.sharding import PartitionSpec as P

MESH = pl.DeviceIdType.MESH
LOG2E = 1.4426950408889634
NEG = -1e30
F32 = jnp.float32
BF16 = jnp.bfloat16
AHEAD = 5
RELAY = 2
FIRST = 2
NT = (((1,), (1,)), ((), ()))


def dot_nt(a, b, **kw):
    return lax.dot_general(a, b, NT, preferred_element_type=F32, **kw)


def dot_nn(a, b, **kw):
    return jnp.dot(a, b, preferred_element_type=F32, **kw)


def kernel(
    sizes,
    q_hbm, k_hbm, v_hbm, do_hbm, table_hbm, ids_hbm, mask_hbm,
    dq_ref, dk_ref, dv_ref, gb_ref,
    kv, qd, tableb, idsb, maskb, byb, biasq, biask,
    ss, sp, dsb, pb, ks, kp, kpb, kdsb, dk0b, dv0b, st, dgb,
    xpart, xbuf, ybuf, zbuf,
    load_sem, small_sem, kv_send, kv_recv, qd_send, qd_mid, qd_far,
    st_send, st_recv, id_send, id_recv, sum_send, sum_recv,
):
    n_seq, nx, ny, nz, n_head, heads, groups = sizes
    T, W = 128, 128
    half = groups // 2
    scale = 0.125
    c = scale * LOG2E
    me = lax.axis_index("seq")
    hi = lax.axis_index("head")
    core = lax.rem(me, 2)
    partner = me + 1 - 2 * core

    def at(offset):
        return lax.rem(me + (offset + n_seq), n_seq)

    row = 2 * nx
    in_row = lax.rem(me, row)
    row_base = me - in_row
    y_at = lax.rem(me // row, ny)
    z_at = me // (row * ny)
    in_plane = lax.rem(me, row * ny)
    halves = heads // 2
    ring_z = n_head * nz * 2
    in_z = (hi * nz + z_at) * 2 + core

    def x_partner(t):
        return row_base + lax.rem(in_row + t, row)

    def y_partner(t):
        return z_at * (row * ny) + lax.rem(y_at + t, ny) * row + in_row

    def z_partner(t):
        w = lax.rem(in_z + t, ring_z)
        w_core = lax.rem(w, 2)
        w_z = lax.rem(w // 2, nz)
        w_head = w // (2 * nz)
        return {"seq": w_z * (row * ny) + in_plane - core + w_core, "head": w_head}

    barrier = pltpu.get_barrier_semaphore()
    partners = [z_partner(t) for t in sorted(range(1, ring_z), key=lambda t: -min(t, ring_z - t))]
    partners += [{"seq": y_partner(t)} for t in range(1, ny)]
    partners += [{"seq": x_partner(t)} for t in range(1, row)]
    partners += [{"seq": at(o)} for o in (1, 2, 3, -1, -2, -3)]
    for other in partners:
        pl.semaphore_signal(barrier, inc=1, device_id=other, device_id_type=MESH)

    def all_of(ref, sem):
        pltpu.make_async_copy(ref, ref, sem).wait()

    srcs = ((q_hbm, qd, 0), (do_hbm, qd, W), (k_hbm, kv, 0), (v_hbm, kv, W))

    def load(n, g):
        src, dst, off = srcs[n]
        return pltpu.make_async_copy(
            src.at[:, pl.ds(g * W, W)], dst.at[g, pl.ds(0, T), pl.ds(off, W)], load_sem.at[n]
        )

    for g in range(groups):
        for n in (2, 3, 0, 1):
            load(n, g).start()
    small = [
        pltpu.make_async_copy(table_hbm, tableb, small_sem.at[0]),
        pltpu.make_async_copy(ids_hbm.at[0], idsb.at[0], small_sem.at[1]),
        pltpu.make_async_copy(mask_hbm, maskb.at[0], small_sem.at[2]),
    ]
    for copy in small:
        copy.start()

    def remote(src, dst, send, recv, device):
        return pltpu.make_async_remote_copy(
            src_ref=src, dst_ref=dst, send_sem=send, recv_sem=recv, device_id=device, device_id_type=MESH
        )

    def slot(buf, g, s):
        return buf.at[g, pl.ds(s * T, T)]

    def kv_copy(n, g):
        if n == 0:
            src, s, device = slot(kv, g, 0), 2, at(2)
        elif n == 1:
            src, s, device = slot(kv, g, 2), 3, at(1)
        else:
            src, s, device = slot(kv, g, pl.multiple_of(2 * core, 2)), 1, partner
        return remote(src, slot(kv, g, s), kv_send.at[n], kv_recv.at[s - 1, g], {"seq": device})

    def qd_copy(n, g):
        if n == 0:
            src, s, device = slot(qd, g, 0), 2, at(-2)
        elif n == 1:
            src, s, device = slot(qd, g, 2), 3, at(-1)
        else:
            src, s, device = slot(qd, g, pl.multiple_of(2 - 2 * core, 2)), 1, partner
        recv = qd_mid.at[g] if s == 2 else qd_far.at[s // 2, g // half]
        return remote(src, slot(qd, g, s), qd_send.at[n], recv, {"seq": device})

    after = n_seq - 1 - me
    kv_sent = (after >= 2, jnp.logical_and(me >= 2, after >= 1), jnp.logical_or(core == 0, me >= 2))
    qd_sent = (me >= 2, jnp.logical_and(after >= 2, me >= 1), jnp.logical_or(core == 1, after >= 2))
    by_slot = {1: 2, 2: 0, 3: 1}

    def kv_start(n, g):
        pl.when(kv_sent[n])(lambda: kv_copy(n, g).start())

    def qd_start(n, g):
        pl.when(qd_sent[n])(lambda: qd_copy(n, g).start())

    def kv_arrived(s, g):
        pl.when(me >= s)(lambda: kv_copy(by_slot[s], g).wait_recv())

    def qd_arrived(g):
        pl.when(after >= 2)(lambda: qd_copy(0, g).wait_recv())

    def st_copy(s, g):
        return remote(st.at[0, g], st.at[s, g], st_send.at[s - 1], st_recv.at[s - 1, g // half], {"seq": at(-s)})

    def id_copy(s):
        return remote(idsb.at[0], idsb.at[s], id_send.at[0, s - 1], id_recv.at[0, s - 1], {"seq": at(-s)})

    def mask_copy(s):
        return remote(maskb.at[0], maskb.at[s], id_send.at[1, s - 1], id_recv.at[1, s - 1], {"seq": at(-s)})

    def send_own(g):
        kv_start(0, g)
        qd_start(0, g)

    def kv_relay(g):
        kv_arrived(2, g)
        kv_start(1, g)
        kv_start(2, g)

    def qd_relay(g):
        qd_arrived(g)
        qd_start(1, g)
        qd_start(2, g)

    with jax.named_scope("load_wait"):
        for copy in small:
            copy.wait()
        for n in (2, 3, 0, 1):
            src, dst, off = srcs[n]
            all_of(dst.at[:, pl.ds(0, T), pl.ds(off, W)], load_sem.at[n])
    with jax.named_scope("barrier"):
        pl.semaphore_wait(barrier, len(partners))
    for s in (1, 2, 3):

        @pl.when(me >= s)
        def _():
            id_copy(s).start()
            mask_copy(s).start()

    for g in range(FIRST):
        send_own(g)
    for s in (1, 2, 3):

        @pl.when(me < s)
        def _():
            kv[:, pl.ds(s * T, T), :] = jnp.zeros((groups, T, 2 * W), BF16)

        @pl.when(after < s)
        def _():
            qd[:, pl.ds(s * T, T), :] = jnp.zeros((groups, T, 2 * W), BF16)
            st[s] = jnp.zeros((groups, 8, T), F32)
            idsb[s] = jnp.zeros((4, 2 * T), jnp.int32)
            maskb[s] = jnp.zeros((1, 4), jnp.int32)

    lane = lax.broadcasted_iota(jnp.int32, (T, T), 1)
    first = lane < 64
    lane8 = lax.broadcasted_iota(jnp.int32, (8, T), 1)
    sub8 = lax.broadcasted_iota(jnp.int32, (8, T), 0)
    codes = lax.broadcasted_iota(jnp.int32, (T, 2 * T), 0)

    def onehot(place, s):
        return (codes == idsb[place, s : s + 1, :]).astype(BF16)

    def thirds(x):
        big = x.astype(BF16)
        rest = x - big.astype(F32)
        mid = rest.astype(BF16)
        return jnp.concatenate([big, mid, (rest - mid.astype(F32)).astype(BF16)], axis=0)

    def whole(x):
        n = x.shape[0] // 3
        return x[:n] + x[n : 2 * n] + x[2 * n :]

    def by_offset(place, s, inside):
        by = whole(dot_nn(thirds(tableb[...] * LOG2E), onehot(place, s)))
        if s:
            keep = jnp.logical_and(maskb[place, 0:1, s : s + 1] == 1, inside)
            by = jnp.where(keep, by, NEG)
        return pltpu.roll(by, 1, 1)

    def skewed(index, head):
        line = jnp.broadcast_to(byb[index, pl.ds(head, 1), :], (8, 2 * T))
        base = pltpu.roll(line, 0, 1, stride=1, stride_axis=0)
        return base[:, :T], base[:, T:]

    def block_row(low, high, a):
        mixed = jnp.where(lane8 >= T - 8 * a, low, high)
        return pltpu.roll(mixed, 8 * a, 1) if a else mixed

    with jax.named_scope("by"):
        for s in range(4):
            byb[s] = by_offset(0, s, me >= s)

    def build_query(g, carry):
        for h in range(2):
            for s in range(4):
                low, high = skewed(s, 2 * g + h)
                for a in range(16):
                    x = block_row(low, high, a)
                    if s == 0:
                        x = jnp.where(8 * a + sub8 <= lane8, x, NEG)
                    biasq[g, pl.ds(s * T + 8 * a, 8), pl.ds(h * T, T)] = x
        return carry

    with jax.named_scope("build_query"):
        lax.fori_loop(0, groups, build_query, 0)
    with jax.named_scope("relay_first"):
        for g in range(RELAY):
            kv_relay(g)
            send_own(FIRST + g)
    for g in range(FIRST + RELAY, AHEAD):
        send_own(g)

    def build_key(g, carry):
        for h in range(2):
            for s in (1, 2, 3):
                low, high = skewed(3 + s, 2 * g + h)
                for a in range(16):
                    biask[g, pl.ds(h * T + 8 * a, 8), pl.ds((s - 1) * T, T)] = block_row(low, high, a)
        return carry

    def build_keys():
        for s in (1, 2, 3):

            @pl.when(after >= s)
            def _():
                id_copy(s).wait_recv()
                mask_copy(s).wait_recv()

            byb[3 + s] = by_offset(s, s, after >= s)
        lax.fori_loop(0, groups, build_key, 0)

    def two(x):
        zero = jnp.zeros_like(x)
        return jnp.concatenate([jnp.where(first, x, zero), jnp.where(first, zero, x)], axis=0)

    def merged(x):
        return jnp.where(first, x[:T], x[T:])

    R = 32

    def fold(x, op):
        parts = [x[8 * j : 8 * j + 8] for j in range(x.shape[0] // 8)]
        return functools.reduce(op, parts)

    def query_side(g):
        q2, do2 = qd[g, 0:T, 0:W], qd[g, 0:T, W : 2 * W]
        ss[...] = dot_nt(kv[g, :, 0:W], two(q2))
        sp[...] = dot_nt(kv[g, :, W : 2 * W], two(do2))
        top = jnp.full((8, 2 * T), NEG, F32)
        for r in range(0, 4 * T, R):
            x = ss[r : r + R] * c + biasq[g, r : r + R]
            ss[r : r + R] = x
            top = jnp.maximum(top, fold(x, jnp.maximum))
        top = top.max(axis=0, keepdims=True)
        total = jnp.zeros((8, 2 * T), F32)
        accum = jnp.zeros((8, 2 * T), F32)
        for r in range(0, 4 * T, R):
            e = jnp.exp2(ss[r : r + R] - top)
            ss[r : r + R] = e
            total = total + fold(e, jnp.add)
            accum = accum + fold(e * sp[r : r + R], jnp.add)
        total = total.sum(axis=0, keepdims=True)
        accum = accum.sum(axis=0, keepdims=True)
        inverse = 1.0 / total
        delta = accum / total
        lse = top + jnp.log2(total)
        st[0, g, 0:1, :] = lse[:, :T]
        st[0, g, 1:2, :] = lse[:, T:]
        st[0, g, 2:3, :] = delta[:, :T]
        st[0, g, 3:4, :] = delta[:, T:]
        for s in range(4):
            low = [jnp.zeros((8, T), F32) for _ in range(2)]
            high = [jnp.zeros((8, T), F32) for _ in range(2)]
            for r in range(s * T, s * T + T, R):
                p = ss[r : r + R] * inverse
                ds = p * (sp[r : r + R] - delta)
                dsb[r : r + R] = ds.astype(BF16)
                if s == 0:
                    pb[r : r + R] = p.astype(BF16)
                for j in range(R // 8):
                    a = (r - s * T) // 8 + j
                    for h in range(2):
                        x = ds[8 * j : 8 * j + 8, h * T : h * T + T]
                        if a:
                            x = pltpu.roll(x, T - 8 * a, 1)
                            here = lane8 < T - 8 * a
                            high[h] = high[h] + jnp.where(here, x, 0.0)
                            low[h] = low[h] + jnp.where(here, 0.0, x)
                        else:
                            high[h] = high[h] + x
            for h in range(2):
                both = jnp.concatenate([low[h], high[h]], axis=1)
                for by in (1, 2, 4):
                    both = both + pltpu.roll(pltpu.roll(both, 2 * T - by, 1), 8 - by, 0)
                dgb[s, pl.ds(2 * g + h, 1), :] = both[0:1]
        turned = dot_nn(kv[g, :, 0:W].T, dsb[...])
        joined = jnp.concatenate([turned[0:64, 0:T], turned[64:T, T : 2 * T]], axis=0)
        dq_ref[:, pl.ds(g * W, W)] = (joined.T * scale).astype(BF16)
        for s in (1, 2, 3):
            pl.when(me >= s)(lambda s=s: st_copy(s, g).start())
        dv0b[g] = jnp.where(first, dot_nn(pb[:, 0:T], do2), dot_nn(pb[:, T : 2 * T], do2))
        dk0b[g] = jnp.where(first, dot_nn(dsb[0:T, 0:T], q2), dot_nn(dsb[0:T, T : 2 * T], q2))

    def key_side(g):
        qs, dos = qd[g, T : 4 * T, 0:W], qd[g, T : 4 * T, W : 2 * W]
        ks[...] = dot_nt(two(kv[g, 0:T, 0:W]), qs)
        kp[...] = dot_nt(two(kv[g, 0:T, W : 2 * W]), dos)
        for h in range(2):
            for s in (1, 2, 3):
                lse = st[s, g, h : h + 1, :]
                delta = st[s, g, 2 + h : 3 + h, :]
                cols = slice((s - 1) * T, s * T)
                for r in range(h * T, h * T + T, R):
                    x = ks[r : r + R, cols] * c + biask[g, r : r + R, cols]
                    p = jnp.exp2(x - lse)
                    ds = p * (kp[r : r + R, cols] - delta)
                    kpb[r : r + R, cols] = p.astype(BF16)
                    kdsb[r : r + R, cols] = ds.astype(BF16)
        dv_ref[:, pl.ds(g * W, W)] = (merged(dot_nn(kpb[...], dos)) + dv0b[g]).astype(BF16)
        dk_ref[:, pl.ds(g * W, W)] = ((merged(dot_nn(kdsb[...], qs)) + dk0b[g]) * scale).astype(BF16)

    def key_ready(part):
        chunks = pl.ds(part * half, half)
        for s in (1, 3):
            pl.when(after >= s)(lambda s=s: all_of(qd.at[chunks, pl.ds(s * T, T)], qd_far.at[s // 2, part]))
        for s in (1, 2, 3):
            pl.when(after >= s)(lambda s=s: all_of(st.at[s, chunks], st_recv.at[s - 1, part]))

    def keys(start, stop):
        def one(g, carry):
            key_side(g)
            return carry

        lax.fori_loop(start, stop, one, 0)

    def step(g, carry):
        with jax.named_scope("relay"):
            pl.when(g + RELAY < groups)(lambda: kv_relay(g + RELAY))
            pl.when(g + AHEAD < groups)(lambda: send_own(g + AHEAD))
            qd_relay(g)
        with jax.named_scope("kv_wait"):
            kv_arrived(3, g)
            kv_arrived(1, g)
        with jax.named_scope("query"):
            query_side(g)
        return carry

    lax.fori_loop(0, groups, step, 0)

    part = jnp.zeros((heads, T), F32)
    with jax.named_scope("buckets"):
        for s in range(4):
            part = part + whole(dot_nt(thirds(pltpu.roll(dgb[s], 2 * T - 1, 1)), onehot(0, s)))
    xpart[...] = part

    def x_copy(t):
        other = x_partner(t)
        start = pl.multiple_of(lax.rem(other, 2) * halves, halves)
        return remote(xpart.at[pl.ds(start, halves)], xbuf.at[in_row], sum_send.at[0], sum_recv.at[0], {"seq": other})

    def y_copy(t):
        return remote(ybuf.at[y_at], ybuf.at[y_at], sum_send.at[1], sum_recv.at[1], {"seq": y_partner(t)})

    def z_copy(t):
        return remote(zbuf.at[in_z], zbuf.at[in_z], sum_send.at[2], sum_recv.at[2], z_partner(t))

    def total_of(buf, slots):
        return functools.reduce(jnp.add, [buf[i] for i in slots])

    for t in range(1, row):
        x_copy(t).start()
    xbuf[in_row] = xpart[pl.ds(pl.multiple_of(core * halves, halves), halves), :]
    with jax.named_scope("build_key"):
        build_keys()
    with jax.named_scope("sum_x"):
        all_of(xbuf.at[pl.ds(0, row - 1)], sum_recv.at[0])
        ybuf[y_at] = total_of(xbuf, range(row))
    for t in range(1, ny):
        y_copy(t).start()
    with jax.named_scope("key_wait"):
        key_ready(0)
    with jax.named_scope("key"):
        keys(0, half - 1)
    with jax.named_scope("sum_y"):
        if ny > 1:
            all_of(ybuf.at[pl.ds(0, ny - 1)], sum_recv.at[1])
        zbuf[in_z] = total_of(ybuf, range(ny))
    for t in range(1, ring_z):
        z_copy(t).start()
    with jax.named_scope("key_wait"):
        key_ready(1)
    with jax.named_scope("key"):
        keys(half - 1, groups)
    with jax.named_scope("sum_z"):
        all_of(zbuf.at[pl.ds(0, ring_z - 1)], sum_recv.at[2])
    for h in range(n_head):
        for side in range(2):
            gb_ref[h * heads + side * halves : h * heads + (side + 1) * halves] = total_of(
                zbuf, [(h * nz + z) * 2 + side for z in range(nz)]
            )

    with jax.named_scope("drain"):
        for n in range(3):
            pl.when(kv_sent[n])(lambda n=n: all_of(kv.at[:, pl.ds(0, T)], kv_send.at[n]))
            pl.when(qd_sent[n])(lambda n=n: all_of(qd.at[:, pl.ds(0, T)], qd_send.at[n]))
        for s in (1, 2, 3):

            @pl.when(me >= s)
            def _():
                all_of(st.at[0], st_send.at[s - 1])
                id_copy(s).wait_send()
                mask_copy(s).wait_send()

        all_of(xbuf.at[pl.ds(0, row - 1)], sum_send.at[0])
        if ny > 1:
            all_of(ybuf.at[pl.ds(0, ny - 1)], sum_send.at[1])
        all_of(zbuf.at[pl.ds(0, ring_z - 1)], sum_send.at[2])


def put_out(*refs):
    sems = refs[8]
    copies = [pltpu.make_async_copy(refs[i], refs[4 + i], sems.at[i]) for i in range(4)]
    for copy in copies:
        copy.start()
    for copy in copies:
        copy.wait()


def solution(mesh):
    n_seq, n_head = mesh.shape["seq"], mesh.shape["head"]
    nx, ny, nz = (4, 4, 4) if n_seq == 128 else (2, 1, 2)

    def body(queries, keys, values, grad_out, bias_table, bucket_ids, block_mask):
        tok, width = queries.shape
        heads, buckets = bias_table.shape
        groups = width // 128
        sizes = (n_seq, nx, ny, nz, n_head, heads, groups)
        row = 2 * nx
        ring_z = n_head * nz * 2
        operands = (queries, keys, values, grad_out, bias_table, bucket_ids, block_mask)
        V = pltpu.VMEM
        dma = pltpu.SemaphoreType.DMA
        scratch = [
            V((groups, 512, 256), BF16), V((groups, 512, 256), BF16),
            V((heads, 128), F32), V((4, 4, 256), jnp.int32), V((4, 1, 4), jnp.int32),
            V((7, heads, 256), F32), V((groups, 512, 256), F32), V((groups, 256, 384), F32),
            V((512, 256), F32), V((512, 256), F32), V((512, 256), BF16), V((128, 256), BF16),
            V((256, 384), F32), V((256, 384), F32), V((256, 384), BF16), V((256, 384), BF16),
            V((groups, 128, 128), F32), V((groups, 128, 128), F32),
            V((4, groups, 8, 128), F32), V((4, heads, 256), F32),
            V((heads, 128), F32), V((row, heads // 2, 128), F32), V((ny, heads // 2, 128), F32),
            V((ring_z, heads // 2, 128), F32),
            dma((4,)), dma((3,)), dma((3,)), dma((3, groups)), dma((3,)), dma((groups,)), dma((2, 2)),
            dma((3,)), dma((3, 2)), dma((2, 3)), dma((2, 3)), dma((3,)), dma((3,)),
        ]
        in_hbm = pl.BlockSpec(memory_space=pltpu.HBM)
        in_vmem = pl.BlockSpec(memory_space=pltpu.VMEM)
        out = jax.ShapeDtypeStruct((tok, width), BF16)
        shapes = (out, out, out, jax.ShapeDtypeStruct((n_head * heads, buckets), F32))
        results = pl.pallas_call(
            functools.partial(kernel, sizes),
            out_shape=shapes,
            in_specs=[in_hbm] * 7,
            out_specs=(in_vmem,) * 4,
            scratch_shapes=scratch,
            compiler_params=pltpu.CompilerParams(
                collective_id=0, has_side_effects=True, vmem_limit_bytes=48 * 1024 * 1024
            ),
        )(*(pltpu.with_memory_space_constraint(x, pltpu.HBM) for x in operands))
        return pl.pallas_call(
            put_out,
            out_shape=shapes,
            in_specs=[in_vmem] * 4,
            out_specs=(pl.BlockSpec(memory_space=pltpu.HBM),) * 4,
            scratch_shapes=[dma((4,))],
        )(*(pltpu.with_memory_space_constraint(x, pltpu.VMEM) for x in results))

    block = P("seq", "head")
    return jax.shard_map(
        body,
        mesh=mesh,
        in_specs=(block, block, block, block, P("head", None), P("seq", None, None), P("seq", None)),
        out_specs=(block, block, block, P(None, None)),
        check_vma=False,
    )
```

```python
import functools

import jax
import jax.numpy as jnp
from jax import lax
from jax.experimental import pallas as pl
from jax.experimental.pallas import tpu as pltpu
from jax.sharding import PartitionSpec as P

MESH = pl.DeviceIdType.MESH
LOG2E = 1.4426950408889634
NEG = -1e30
F32 = jnp.float32
BF16 = jnp.bfloat16
AHEAD = 5
RELAY = 2
FIRST = 2
NT = (((1,), (1,)), ((), ()))


def dot_nt(a, b, **kw):
    return lax.dot_general(a, b, NT, preferred_element_type=F32, **kw)


def dot_nn(a, b, **kw):
    return jnp.dot(a, b, preferred_element_type=F32, **kw)


def kernel(
    sizes,
    q_hbm, k_hbm, v_hbm, do_hbm, table_hbm, ids_hbm, mask_hbm,
    dq_ref, dk_ref, dv_ref, gb_ref,
    kv, qd, tableb, idsb, maskb, byb, biasq, biask,
    ss, sp, dsb, pb, ks, kp, kpb, kdsb, dk0b, dv0b, st, dgb,
    xpart, xbuf, ybuf, zbuf,
    load_sem, small_sem, kv_send, kv_recv, qd_send, qd_mid, qd_far,
    st_send, st_recv, id_send, id_recv, sum_send, sum_recv,
):
    n_seq, nx, ny, nz, n_head, heads, groups = sizes
    T, W = 128, 128
    half = groups // 2
    scale = 0.125
    c = scale * LOG2E
    me = lax.axis_index("seq")
    hi = lax.axis_index("head")
    core = lax.rem(me, 2)
    partner = me + 1 - 2 * core

    def at(offset):
        return lax.rem(me + (offset + n_seq), n_seq)

    row = 2 * nx
    in_row = lax.rem(me, row)
    row_base = me - in_row
    y_at = lax.rem(me // row, ny)
    z_at = me // (row * ny)
    in_plane = lax.rem(me, row * ny)
    halves = heads // 2
    ring_z = n_head * nz * 2
    in_z = (hi * nz + z_at) * 2 + core

    def x_partner(t):
        return row_base + lax.rem(in_row + t, row)

    def y_partner(t):
        return z_at * (row * ny) + lax.rem(y_at + t, ny) * row + in_row

    def z_partner(t):
        w = lax.rem(in_z + t, ring_z)
        w_core = lax.rem(w, 2)
        w_z = lax.rem(w // 2, nz)
        w_head = w // (2 * nz)
        return {"seq": w_z * (row * ny) + in_plane - core + w_core, "head": w_head}

    def all_of(ref, sem):
        pltpu.make_async_copy(ref, ref, sem).wait()

    srcs = ((k_hbm, kv, 0, 0), (v_hbm, kv, W, 0), (q_hbm, qd, 0, 1), (do_hbm, qd, W, 1))

    def load(chunks, part):
        for g in chunks:
            for src, dst, off, n in srcs:
                pltpu.make_async_copy(
                    src.at[:, pl.ds(g * W, W)], dst.at[g, pl.ds(0, T), pl.ds(off, W)], load_sem.at[part, n]
                ).start()

    def loaded(start, count, part):
        for n, buf in enumerate((kv, qd)):
            all_of(buf.at[pl.ds(start, count), pl.ds(0, T)], load_sem.at[part, n])

    load(range(FIRST), 0)
    small = [
        pltpu.make_async_copy(table_hbm, tableb, small_sem.at[0]),
        pltpu.make_async_copy(ids_hbm.at[0], idsb.at[0], small_sem.at[1]),
        pltpu.make_async_copy(mask_hbm, maskb.at[0], small_sem.at[2]),
    ]
    for copy in small:
        copy.start()

    def far_first(count):
        return sorted(range(1, count), key=lambda t: -min(t, count - t))

    barrier = pltpu.get_barrier_semaphore()
    partners = [z_partner(t) for t in far_first(ring_z)]
    partners += [{"seq": y_partner(t)} for t in far_first(ny)]
    partners += [{"seq": x_partner(t)} for t in far_first(row)]
    partners += [{"seq": at(o)} for o in (3, -3, 2, -2, 1, -1)]
    for other in partners:
        pl.semaphore_signal(barrier, inc=1, device_id=other, device_id_type=MESH)
    load(range(FIRST, groups), 1)

    def remote(src, dst, send, recv, device):
        return pltpu.make_async_remote_copy(
            src_ref=src, dst_ref=dst, send_sem=send, recv_sem=recv, device_id=device, device_id_type=MESH
        )

    def slot(buf, g, s):
        return buf.at[g, pl.ds(s * T, T)]

    def kv_copy(n, g):
        if n == 0:
            src, s, device = slot(kv, g, 0), 2, at(2)
        elif n == 1:
            src, s, device = slot(kv, g, 2), 3, at(1)
        else:
            src, s, device = slot(kv, g, pl.multiple_of(2 * core, 2)), 1, partner
        return remote(src, slot(kv, g, s), kv_send.at[n], kv_recv.at[s - 1, g], {"seq": device})

    def qd_copy(n, g):
        if n == 0:
            src, s, device = slot(qd, g, 0), 2, at(-2)
        elif n == 1:
            src, s, device = slot(qd, g, 2), 3, at(-1)
        else:
            src, s, device = slot(qd, g, pl.multiple_of(2 - 2 * core, 2)), 1, partner
        recv = qd_mid.at[g] if s == 2 else qd_far.at[s // 2, g // half]
        return remote(src, slot(qd, g, s), qd_send.at[n], recv, {"seq": device})

    after = n_seq - 1 - me
    kv_sent = (after >= 2, jnp.logical_and(me >= 2, after >= 1), jnp.logical_or(core == 0, me >= 2))
    qd_sent = (me >= 2, jnp.logical_and(after >= 2, me >= 1), jnp.logical_or(core == 1, after >= 2))
    by_slot = {1: 2, 2: 0, 3: 1}

    def kv_start(n, g):
        pl.when(kv_sent[n])(lambda: kv_copy(n, g).start())

    def qd_start(n, g):
        pl.when(qd_sent[n])(lambda: qd_copy(n, g).start())

    def kv_arrived(s, g):
        pl.when(me >= s)(lambda: kv_copy(by_slot[s], g).wait_recv())

    def qd_arrived(g):
        pl.when(after >= 2)(lambda: qd_copy(0, g).wait_recv())

    def st_copy(s, g):
        return remote(st.at[0, g], st.at[s, g], st_send.at[s - 1], st_recv.at[s - 1, g // half], {"seq": at(-s)})

    def id_copy(s):
        return remote(idsb.at[0], idsb.at[s], id_send.at[0, s - 1], id_recv.at[0, s - 1], {"seq": at(-s)})

    def mask_copy(s):
        return remote(maskb.at[0], maskb.at[s], id_send.at[1, s - 1], id_recv.at[1, s - 1], {"seq": at(-s)})

    def send_own(g):
        kv_start(0, g)
        qd_start(0, g)

    def kv_relay(g):
        kv_arrived(2, g)
        kv_start(1, g)
        kv_start(2, g)

    def qd_relay(g):
        qd_arrived(g)
        qd_start(1, g)
        qd_start(2, g)

    with jax.named_scope("load_wait"):
        loaded(0, FIRST, 0)
        for copy in small:
            copy.wait()
    with jax.named_scope("barrier"):
        pl.semaphore_wait(barrier, len(partners))
    for s in (1, 2, 3):

        @pl.when(me >= s)
        def _():
            id_copy(s).start()
            mask_copy(s).start()

    for g in range(FIRST):
        send_own(g)
    loaded(FIRST, groups - FIRST, 1)
    for s in (1, 2, 3):

        @pl.when(me < s)
        def _():
            kv[:, pl.ds(s * T, T), :] = jnp.zeros((groups, T, 2 * W), BF16)

        @pl.when(after < s)
        def _():
            qd[:, pl.ds(s * T, T), :] = jnp.zeros((groups, T, 2 * W), BF16)
            st[s] = jnp.zeros((groups, 8, T), F32)
            idsb[s] = jnp.zeros((4, 2 * T), jnp.int32)
            maskb[s] = jnp.zeros((1, 4), jnp.int32)

    lane = lax.broadcasted_iota(jnp.int32, (T, T), 1)
    first = lane < 64
    lane8 = lax.broadcasted_iota(jnp.int32, (8, T), 1)
    sub8 = lax.broadcasted_iota(jnp.int32, (8, T), 0)
    codes = lax.broadcasted_iota(jnp.int32, (T, 2 * T), 0)

    def onehot(place, s):
        return (codes == idsb[place, s : s + 1, :]).astype(BF16)

    def thirds(x):
        big = x.astype(BF16)
        rest = x - big.astype(F32)
        mid = rest.astype(BF16)
        return jnp.concatenate([big, mid, (rest - mid.astype(F32)).astype(BF16)], axis=0)

    def whole(x):
        n = x.shape[0] // 3
        return x[:n] + x[n : 2 * n] + x[2 * n :]

    def by_offset(place, s, inside):
        by = whole(dot_nn(thirds(tableb[...] * LOG2E), onehot(place, s)))
        if s:
            keep = jnp.logical_and(maskb[place, 0:1, s : s + 1] == 1, inside)
            by = jnp.where(keep, by, NEG)
        return pltpu.roll(by, 1, 1)

    def skewed(index, head):
        line = jnp.broadcast_to(byb[index, pl.ds(head, 1), :], (8, 2 * T))
        base = pltpu.roll(line, 0, 1, stride=1, stride_axis=0)
        return base[:, :T], base[:, T:]

    def block_row(low, high, a):
        mixed = jnp.where(lane8 >= T - 8 * a, low, high)
        return pltpu.roll(mixed, 8 * a, 1) if a else mixed

    with jax.named_scope("by"):
        for s in range(4):
            byb[s] = by_offset(0, s, me >= s)

    def build_query(g, carry):
        for h in range(2):
            for s in range(4):
                low, high = skewed(s, 2 * g + h)
                for a in range(16):
                    x = block_row(low, high, a)
                    if s == 0:
                        x = jnp.where(8 * a + sub8 <= lane8, x, NEG)
                    biasq[g, pl.ds(s * T + 8 * a, 8), pl.ds(h * T, T)] = x
        return carry

    with jax.named_scope("build_query"):
        lax.fori_loop(0, groups, build_query, 0)
    send_own(FIRST)
    with jax.named_scope("relay_first"):
        for g in range(RELAY):
            kv_relay(g)
            send_own(FIRST + 1 + g)

    def build_key(g, carry):
        for h in range(2):
            for s in (1, 2, 3):
                low, high = skewed(3 + s, 2 * g + h)
                for a in range(16):
                    biask[g, pl.ds(h * T + 8 * a, 8), pl.ds((s - 1) * T, T)] = block_row(low, high, a)
        return carry

    with jax.named_scope("by_key"):
        for s in (1, 2, 3):

            @pl.when(after >= s)
            def _():
                id_copy(s).wait_recv()
                mask_copy(s).wait_recv()

            byb[3 + s] = by_offset(s, s, after >= s)

    def two(x):
        zero = jnp.zeros_like(x)
        return jnp.concatenate([jnp.where(first, x, zero), jnp.where(first, zero, x)], axis=0)

    def merged(x):
        return jnp.where(first, x[:T], x[T:])

    R = 32

    def fold(x, op):
        parts = [x[8 * j : 8 * j + 8] for j in range(x.shape[0] // 8)]
        return functools.reduce(op, parts)

    def query_scores(g):
        q2, do2 = qd[g, 0:T, 0:W], qd[g, 0:T, W : 2 * W]
        ss[...] = dot_nt(kv[g, :, 0:W], two(q2))
        sp[...] = dot_nt(kv[g, :, W : 2 * W], two(do2))
        top = jnp.full((8, 2 * T), NEG, F32)
        for r in range(0, 4 * T, R):
            x = ss[r : r + R] * c + biasq[g, r : r + R]
            ss[r : r + R] = x
            top = jnp.maximum(top, fold(x, jnp.maximum))
        top = top.max(axis=0, keepdims=True)
        total = jnp.zeros((8, 2 * T), F32)
        accum = jnp.zeros((8, 2 * T), F32)
        for r in range(0, 4 * T, R):
            e = jnp.exp2(ss[r : r + R] - top)
            ss[r : r + R] = e
            total = total + fold(e, jnp.add)
            accum = accum + fold(e * sp[r : r + R], jnp.add)
        total = total.sum(axis=0, keepdims=True)
        accum = accum.sum(axis=0, keepdims=True)
        inverse = 1.0 / total
        delta = accum / total
        lse = top + jnp.log2(total)
        st[0, g, 0:1, :] = lse[:, :T]
        st[0, g, 1:2, :] = lse[:, T:]
        st[0, g, 2:3, :] = delta[:, :T]
        st[0, g, 3:4, :] = delta[:, T:]
        for s in range(4):
            low = [jnp.zeros((8, T), F32) for _ in range(2)]
            high = [jnp.zeros((8, T), F32) for _ in range(2)]
            for r in range(s * T, s * T + T, R):
                p = ss[r : r + R] * inverse
                ds = p * (sp[r : r + R] - delta)
                dsb[r : r + R] = ds.astype(BF16)
                if s == 0:
                    pb[r : r + R] = p.astype(BF16)
                for j in range(R // 8):
                    a = (r - s * T) // 8 + j
                    for h in range(2):
                        x = ds[8 * j : 8 * j + 8, h * T : h * T + T]
                        if a:
                            x = pltpu.roll(x, T - 8 * a, 1)
                            here = lane8 < T - 8 * a
                            high[h] = high[h] + jnp.where(here, x, 0.0)
                            low[h] = low[h] + jnp.where(here, 0.0, x)
                        else:
                            high[h] = high[h] + x
            for h in range(2):
                both = jnp.concatenate([low[h], high[h]], axis=1)
                for by in (1, 2, 4):
                    both = both + pltpu.roll(pltpu.roll(both, 2 * T - by, 1), 8 - by, 0)
                dgb[s, pl.ds(2 * g + h, 1), :] = both[0:1]

    def query_grads(g):
        q2, do2 = qd[g, 0:T, 0:W], qd[g, 0:T, W : 2 * W]
        turned = dot_nn(kv[g, :, 0:W].T, dsb[...])
        joined = jnp.concatenate([turned[0:64, 0:T], turned[64:T, T : 2 * T]], axis=0)
        dq_ref[:, pl.ds(g * W, W)] = (joined.T * scale).astype(BF16)
        for s in (1, 2, 3):
            pl.when(me >= s)(lambda s=s: st_copy(s, g).start())
        dv0b[g] = jnp.where(first, dot_nn(pb[:, 0:T], do2), dot_nn(pb[:, T : 2 * T], do2))
        dk0b[g] = jnp.where(first, dot_nn(dsb[0:T, 0:T], q2), dot_nn(dsb[0:T, T : 2 * T], q2))

    def key_side(g):
        qs, dos = qd[g, T : 4 * T, 0:W], qd[g, T : 4 * T, W : 2 * W]
        ks[...] = dot_nt(two(kv[g, 0:T, 0:W]), qs)
        kp[...] = dot_nt(two(kv[g, 0:T, W : 2 * W]), dos)
        for h in range(2):
            for s in (1, 2, 3):
                lse = st[s, g, h : h + 1, :]
                delta = st[s, g, 2 + h : 3 + h, :]
                cols = slice((s - 1) * T, s * T)
                for r in range(h * T, h * T + T, R):
                    x = ks[r : r + R, cols] * c + biask[g, r : r + R, cols]
                    p = jnp.exp2(x - lse)
                    ds = p * (kp[r : r + R, cols] - delta)
                    kpb[r : r + R, cols] = p.astype(BF16)
                    kdsb[r : r + R, cols] = ds.astype(BF16)
        dv_ref[:, pl.ds(g * W, W)] = (merged(dot_nn(kpb[...], dos)) + dv0b[g]).astype(BF16)
        dk_ref[:, pl.ds(g * W, W)] = ((merged(dot_nn(kdsb[...], qs)) + dk0b[g]) * scale).astype(BF16)

    def key_ready(part):
        chunks = pl.ds(part * half, half)
        for s in (1, 3):
            pl.when(after >= s)(lambda s=s: all_of(qd.at[chunks, pl.ds(s * T, T)], qd_far.at[s // 2, part]))
        for s in (1, 2, 3):
            pl.when(after >= s)(lambda s=s: all_of(st.at[s, chunks], st_recv.at[s - 1, part]))

    def keys(start, stop):
        def one(g, carry):
            key_side(g)
            return carry

        lax.fori_loop(start, stop, one, 0)

    def step(g, carry):
        with jax.named_scope("relay"):
            pl.when(g + RELAY < groups)(lambda: kv_relay(g + RELAY))
            pl.when(g + AHEAD < groups)(lambda: send_own(g + AHEAD))
            qd_relay(g)
        with jax.named_scope("kv_wait"):
            kv_arrived(3, g)
            kv_arrived(1, g)
        with jax.named_scope("query"):
            query_scores(g)
            query_grads(g)
        return carry

    lax.fori_loop(0, groups - 1, step, 0)
    qd_relay(groups - 1)
    with jax.named_scope("kv_wait"):
        kv_arrived(3, groups - 1)
        kv_arrived(1, groups - 1)
    with jax.named_scope("query"):
        query_scores(groups - 1)

    part = jnp.zeros((heads, T), F32)
    with jax.named_scope("buckets"):
        for s in range(4):
            part = part + whole(dot_nt(thirds(pltpu.roll(dgb[s], 2 * T - 1, 1)), onehot(0, s)))
    xpart[...] = part

    def x_copy(t):
        other = x_partner(t)
        start = pl.multiple_of(lax.rem(other, 2) * halves, halves)
        return remote(xpart.at[pl.ds(start, halves)], xbuf.at[in_row], sum_send.at[0], sum_recv.at[0], {"seq": other})

    def y_copy(t):
        return remote(ybuf.at[y_at], ybuf.at[y_at], sum_send.at[1], sum_recv.at[1], {"seq": y_partner(t)})

    def z_copy(t):
        return remote(zbuf.at[in_z], zbuf.at[in_z], sum_send.at[2], sum_recv.at[2], z_partner(t))

    def total_of(buf, slots):
        return functools.reduce(jnp.add, [buf[i] for i in slots])

    for t in far_first(row):
        x_copy(t).start()
    xbuf[in_row] = xpart[pl.ds(pl.multiple_of(core * halves, halves), halves), :]
    with jax.named_scope("grads"):
        query_grads(groups - 1)
    with jax.named_scope("build_key"):
        lax.fori_loop(0, groups, build_key, 0)
    with jax.named_scope("sum_x"):
        all_of(xbuf.at[pl.ds(0, row - 1)], sum_recv.at[0])
        ybuf[y_at] = total_of(xbuf, range(row))
    for t in far_first(ny):
        y_copy(t).start()
    with jax.named_scope("key_wait"):
        key_ready(0)
    with jax.named_scope("key"):
        keys(0, 2)
    with jax.named_scope("sum_y"):
        if ny > 1:
            all_of(ybuf.at[pl.ds(0, ny - 1)], sum_recv.at[1])
        zbuf[in_z] = total_of(ybuf, range(ny))
    for t in far_first(ring_z):
        z_copy(t).start()
    with jax.named_scope("key_wait"):
        key_ready(1)
    with jax.named_scope("key"):
        keys(2, groups)
    with jax.named_scope("sum_z"):
        all_of(zbuf.at[pl.ds(0, ring_z - 1)], sum_recv.at[2])
    for h in range(n_head):
        for side in range(2):
            gb_ref[h * heads + side * halves : h * heads + (side + 1) * halves] = total_of(
                zbuf, [(h * nz + z) * 2 + side for z in range(nz)]
            )

    with jax.named_scope("drain"):
        for n in range(3):
            pl.when(kv_sent[n])(lambda n=n: all_of(kv.at[:, pl.ds(0, T)], kv_send.at[n]))
            pl.when(qd_sent[n])(lambda n=n: all_of(qd.at[:, pl.ds(0, T)], qd_send.at[n]))
        for s in (1, 2, 3):

            @pl.when(me >= s)
            def _():
                all_of(st.at[0], st_send.at[s - 1])
                id_copy(s).wait_send()
                mask_copy(s).wait_send()

        all_of(xbuf.at[pl.ds(0, row - 1)], sum_send.at[0])
        if ny > 1:
            all_of(ybuf.at[pl.ds(0, ny - 1)], sum_send.at[1])
        all_of(zbuf.at[pl.ds(0, ring_z - 1)], sum_send.at[2])


def put_out(*refs):
    sems = refs[8]
    copies = [pltpu.make_async_copy(refs[i], refs[4 + i], sems.at[i]) for i in range(4)]
    for copy in copies:
        copy.start()
    for copy in copies:
        copy.wait()


def solution(mesh):
    n_seq, n_head = mesh.shape["seq"], mesh.shape["head"]
    nx, ny, nz = (4, 4, 4) if n_seq == 128 else (2, 1, 2)

    def body(queries, keys, values, grad_out, bias_table, bucket_ids, block_mask):
        tok, width = queries.shape
        heads, buckets = bias_table.shape
        groups = width // 128
        sizes = (n_seq, nx, ny, nz, n_head, heads, groups)
        row = 2 * nx
        ring_z = n_head * nz * 2
        operands = (queries, keys, values, grad_out, bias_table, bucket_ids, block_mask)
        V = pltpu.VMEM
        dma = pltpu.SemaphoreType.DMA
        scratch = [
            V((groups, 512, 256), BF16), V((groups, 512, 256), BF16),
            V((heads, 128), F32), V((4, 4, 256), jnp.int32), V((4, 1, 4), jnp.int32),
            V((7, heads, 256), F32), V((groups, 512, 256), F32), V((groups, 256, 384), F32),
            V((512, 256), F32), V((512, 256), F32), V((512, 256), BF16), V((128, 256), BF16),
            V((256, 384), F32), V((256, 384), F32), V((256, 384), BF16), V((256, 384), BF16),
            V((groups, 128, 128), F32), V((groups, 128, 128), F32),
            V((4, groups, 8, 128), F32), V((4, heads, 256), F32),
            V((heads, 128), F32), V((row, heads // 2, 128), F32), V((ny, heads // 2, 128), F32),
            V((ring_z, heads // 2, 128), F32),
            dma((2, 2)), dma((3,)), dma((3,)), dma((3, groups)), dma((3,)), dma((groups,)), dma((2, 2)),
            dma((3,)), dma((3, 2)), dma((2, 3)), dma((2, 3)), dma((3,)), dma((3,)),
        ]
        in_hbm = pl.BlockSpec(memory_space=pltpu.HBM)
        in_vmem = pl.BlockSpec(memory_space=pltpu.VMEM)
        out = jax.ShapeDtypeStruct((tok, width), BF16)
        shapes = (out, out, out, jax.ShapeDtypeStruct((n_head * heads, buckets), F32))
        results = pl.pallas_call(
            functools.partial(kernel, sizes),
            out_shape=shapes,
            in_specs=[in_hbm] * 7,
            out_specs=(in_vmem,) * 4,
            scratch_shapes=scratch,
            compiler_params=pltpu.CompilerParams(
                collective_id=0, has_side_effects=True, vmem_limit_bytes=48 * 1024 * 1024
            ),
        )(*(pltpu.with_memory_space_constraint(x, pltpu.HBM) for x in operands))
        return pl.pallas_call(
            put_out,
            out_shape=shapes,
            in_specs=[in_vmem] * 4,
            out_specs=(pl.BlockSpec(memory_space=pltpu.HBM),) * 4,
            scratch_shapes=[dma((4,))],
        )(*(pltpu.with_memory_space_constraint(x, pltpu.VMEM) for x in results))

    block = P("seq", "head")
    return jax.shard_map(
        body,
        mesh=mesh,
        in_specs=(block, block, block, block, P("head", None), P("seq", None, None), P("seq", None)),
        out_specs=(block, block, block, P(None, None)),
        check_vma=False,
    )
```

```python
import functools

import jax
import jax.numpy as jnp
from jax import lax
from jax.experimental import pallas as pl
from jax.experimental.pallas import tpu as pltpu
from jax.sharding import PartitionSpec as P

MESH = pl.DeviceIdType.MESH
LOG2E = 1.4426950408889634
NEG = -1e30
F32 = jnp.float32
BF16 = jnp.bfloat16
AHEAD = 5
RELAY = 2
FIRST = 3
DEFER = 4
LAST_KEY = 7
NT = (((1,), (1,)), ((), ()))


def dot_nt(a, b, **kw):
    return lax.dot_general(a, b, NT, preferred_element_type=F32, **kw)


def dot_nn(a, b, **kw):
    return jnp.dot(a, b, preferred_element_type=F32, **kw)


def kernel(
    sizes,
    q_hbm, k_hbm, v_hbm, do_hbm, table_hbm, ids_hbm, mask_hbm,
    dq_ref, dk_ref, dv_ref, gb_ref,
    kv, qd, tableb, idsb, maskb, byb, biasq, biask,
    ss, sp, dsb, pb, ks, kp, kpb, kdsb, dk0b, dv0b, st, dgb,
    xpart, xpair, xbuf, ybuf, zbuf, gbuf,
    load_sem, small_sem, kv_send, kv_recv, qd_send, qd_mid, qd_far,
    st_send, st_recv, id_send, id_recv, sum_send, sum_recv,
):
    n_seq, nx, ny, nz, n_head, heads, groups = sizes
    T, W = 128, 128
    half = groups // 2
    scale = 0.125
    c = scale * LOG2E
    me = lax.axis_index("seq")
    hi = lax.axis_index("head")
    core = lax.rem(me, 2)
    partner = me + 1 - 2 * core

    def at(offset):
        return lax.rem(me + (offset + n_seq), n_seq)

    row = 2 * nx
    x_at = lax.rem(me, row) // 2
    y_at = lax.rem(me // row, ny)
    z_at = me // (row * ny)
    ring_z = n_head * nz
    in_z = hi * nz + z_at

    def x_partner(t):
        return {"seq": me + 2 * (lax.rem(x_at + t, nx) - x_at)}

    def y_partner(t):
        return {"seq": me + row * (lax.rem(y_at + t, ny) - y_at)}

    def z_partner(t):
        w = lax.rem(in_z + t, ring_z)
        return {"seq": me + row * ny * (lax.rem(w, nz) - z_at), "head": w // nz}

    def far_first(count):
        return sorted(range(1, count), key=lambda t: -min(t, count - t))

    barrier = pltpu.get_barrier_semaphore()

    def signal(other):
        pl.semaphore_signal(barrier, inc=1, device_id=other, device_id_type=MESH)

    @pl.when(core == 1)
    def _():
        for t in far_first(ring_z):
            signal(z_partner(t))

    def all_of(ref, sem):
        pltpu.make_async_copy(ref, ref, sem).wait()

    srcs = ((k_hbm, kv, 0, 0), (v_hbm, kv, W, 0), (q_hbm, qd, 0, 1), (do_hbm, qd, W, 1))

    def load(chunks, part):
        for g in chunks:
            for src, dst, off, n in srcs:
                pltpu.make_async_copy(
                    src.at[:, pl.ds(g * W, W)], dst.at[g, pl.ds(0, T), pl.ds(off, W)], load_sem.at[part, n]
                ).start()

    def loaded(start, count, part):
        for n, buf in enumerate((kv, qd)):
            all_of(buf.at[pl.ds(start, count), pl.ds(0, T)], load_sem.at[part, n])

    load(range(FIRST), 0)
    small = [
        pltpu.make_async_copy(table_hbm, tableb, small_sem.at[0]),
        pltpu.make_async_copy(ids_hbm.at[0], idsb.at[0], small_sem.at[1]),
        pltpu.make_async_copy(mask_hbm, maskb.at[0], small_sem.at[2]),
    ]
    for copy in small:
        copy.start()

    @pl.when(core == 1)
    def _():
        for t in far_first(ny):
            signal(y_partner(t))
        for t in far_first(nx):
            signal(x_partner(t))

    near = jnp.minimum(me, 3) + jnp.minimum(n_seq - 1 - me, 3)
    for o in (3, 2, 1):
        pl.when(me >= o)(lambda o=o: signal({"seq": me - o}))
        pl.when(me + o < n_seq)(lambda o=o: signal({"seq": me + o}))
    load(range(FIRST, groups), 1)

    def remote(src, dst, send, recv, device):
        return pltpu.make_async_remote_copy(
            src_ref=src, dst_ref=dst, send_sem=send, recv_sem=recv, device_id=device, device_id_type=MESH
        )

    def slot(buf, g, s):
        return buf.at[g, pl.ds(s * T, T)]

    def kv_copy(n, g):
        if n == 0:
            src, s, device = slot(kv, g, 0), 2, at(2)
        elif n == 1:
            src, s, device = slot(kv, g, 2), 3, at(1)
        else:
            src, s, device = slot(kv, g, pl.multiple_of(2 * core, 2)), 1, partner
        return remote(src, slot(kv, g, s), kv_send.at[n], kv_recv.at[s - 1, g], {"seq": device})

    def qd_copy(n, g):
        if n == 0:
            src, s, device = slot(qd, g, 0), 2, at(-2)
        elif n == 1:
            src, s, device = slot(qd, g, 2), 3, at(-1)
        else:
            src, s, device = slot(qd, g, pl.multiple_of(2 - 2 * core, 2)), 1, partner
        recv = qd_mid.at[g] if s == 2 else qd_far.at[s // 2, g // half]
        return remote(src, slot(qd, g, s), qd_send.at[n], recv, {"seq": device})

    after = n_seq - 1 - me
    kv_sent = (after >= 2, jnp.logical_and(me >= 2, after >= 1), jnp.logical_or(core == 0, me >= 2))
    qd_sent = (me >= 2, jnp.logical_and(after >= 2, me >= 1), jnp.logical_or(core == 1, after >= 2))
    by_slot = {1: 2, 2: 0, 3: 1}

    def kv_start(n, g):
        pl.when(kv_sent[n])(lambda: kv_copy(n, g).start())

    def qd_start(n, g):
        pl.when(qd_sent[n])(lambda: qd_copy(n, g).start())

    def kv_arrived(s, g):
        pl.when(me >= s)(lambda: kv_copy(by_slot[s], g).wait_recv())

    def qd_arrived(g):
        pl.when(after >= 2)(lambda: qd_copy(0, g).wait_recv())

    def st_copy(s, g):
        return remote(st.at[0, g], st.at[s, g], st_send.at[s - 1], st_recv.at[s - 1, g // half], {"seq": at(-s)})

    def id_copy(s):
        return remote(idsb.at[0], idsb.at[s], id_send.at[0, s - 1], id_recv.at[0, s - 1], {"seq": at(-s)})

    def mask_copy(s):
        return remote(maskb.at[0], maskb.at[s], id_send.at[1, s - 1], id_recv.at[1, s - 1], {"seq": at(-s)})

    def send_own(g):
        kv_start(0, g)
        qd_start(0, g)

    def kv_relay(g):
        kv_arrived(2, g)
        kv_start(1, g)
        kv_start(2, g)

    def qd_relay(g):
        qd_arrived(g)
        qd_start(1, g)
        qd_start(2, g)

    with jax.named_scope("load_wait"):
        loaded(0, FIRST, 0)
        for copy in small:
            copy.wait()
    with jax.named_scope("barrier"):
        pl.semaphore_wait(barrier, near + core * (ring_z + ny + nx - 3))
    for s in (1, 2, 3):

        @pl.when(me >= s)
        def _():
            id_copy(s).start()
            mask_copy(s).start()

    for g in range(FIRST):
        send_own(g)
    loaded(FIRST, groups - FIRST, 1)
    for s in (1, 2, 3):

        @pl.when(me < s)
        def _():
            kv[:, pl.ds(s * T, T), :] = jnp.zeros((groups, T, 2 * W), BF16)

        @pl.when(after < s)
        def _():
            qd[:, pl.ds(s * T, T), :] = jnp.zeros((groups, T, 2 * W), BF16)
            st[s] = jnp.zeros((groups, 8, T), F32)
            idsb[s] = jnp.zeros((4, 2 * T), jnp.int32)
            maskb[s] = jnp.zeros((1, 4), jnp.int32)

    lane = lax.broadcasted_iota(jnp.int32, (T, T), 1)
    first = lane < 64
    lane8 = lax.broadcasted_iota(jnp.int32, (8, T), 1)
    sub8 = lax.broadcasted_iota(jnp.int32, (8, T), 0)
    codes = lax.broadcasted_iota(jnp.int32, (T, 2 * T), 0)

    def onehot(place, s):
        return (codes == idsb[place, s : s + 1, :]).astype(BF16)

    def thirds(x):
        big = x.astype(BF16)
        rest = x - big.astype(F32)
        mid = rest.astype(BF16)
        return jnp.concatenate([big, mid, (rest - mid.astype(F32)).astype(BF16)], axis=0)

    def whole(x):
        n = x.shape[0] // 3
        return x[:n] + x[n : 2 * n] + x[2 * n :]

    def by_offset(place, s, inside):
        by = whole(dot_nn(thirds(tableb[...] * LOG2E), onehot(place, s)))
        if s:
            keep = jnp.logical_and(maskb[place, 0:1, s : s + 1] == 1, inside)
            by = jnp.where(keep, by, NEG)
        return pltpu.roll(by, 1, 1)

    def skewed(index, head):
        line = jnp.broadcast_to(byb[index, pl.ds(head, 1), :], (8, 2 * T))
        base = pltpu.roll(line, 0, 1, stride=1, stride_axis=0)
        return base[:, :T], base[:, T:]

    def block_row(low, high, a):
        mixed = jnp.where(lane8 >= T - 8 * a, low, high)
        return pltpu.roll(mixed, 8 * a, 1) if a else mixed

    with jax.named_scope("by"):
        for s in range(4):
            byb[s] = by_offset(0, s, me >= s)

    def build_query(g, carry):
        for h in range(2):
            for s in range(4):
                low, high = skewed(s, 2 * g + h)
                for a in range(16):
                    x = block_row(low, high, a)
                    if s == 0:
                        x = jnp.where(8 * a + sub8 <= lane8, x, NEG)
                    biasq[g, pl.ds(s * T + 8 * a, 8), pl.ds(h * T, T)] = x
        return carry

    with jax.named_scope("build_query"):
        lax.fori_loop(0, groups, build_query, 0)
    send_own(FIRST)
    with jax.named_scope("relay_first"):
        for g in range(RELAY):
            kv_relay(g)
            if FIRST + 1 + g < AHEAD:
                send_own(FIRST + 1 + g)

    def build_key(g, carry):
        for h in range(2):
            for s in (1, 2, 3):
                low, high = skewed(3 + s, 2 * g + h)
                for a in range(16):
                    biask[g, pl.ds(h * T + 8 * a, 8), pl.ds((s - 1) * T, T)] = block_row(low, high, a)
        return carry

    with jax.named_scope("by_key"):
        for s in (1, 2, 3):

            @pl.when(after >= s)
            def _():
                id_copy(s).wait_recv()
                mask_copy(s).wait_recv()

            byb[3 + s] = by_offset(s, s, after >= s)

    def two(x):
        zero = jnp.zeros_like(x)
        return jnp.concatenate([jnp.where(first, x, zero), jnp.where(first, zero, x)], axis=0)

    def merged(x):
        return jnp.where(first, x[:T], x[T:])

    R = 32

    def fold(x, op):
        parts = [x[8 * j : 8 * j + 8] for j in range(x.shape[0] // 8)]
        return functools.reduce(op, parts)

    def query_scores(g):
        q2, do2 = qd[g, 0:T, 0:W], qd[g, 0:T, W : 2 * W]
        ss[...] = dot_nt(kv[g, :, 0:W], two(q2))
        sp[...] = dot_nt(kv[g, :, W : 2 * W], two(do2))
        top = jnp.full((8, 2 * T), NEG, F32)
        for r in range(0, 4 * T, R):
            x = ss[r : r + R] * c + biasq[g, r : r + R]
            ss[r : r + R] = x
            top = jnp.maximum(top, fold(x, jnp.maximum))
        top = top.max(axis=0, keepdims=True)
        total = jnp.zeros((8, 2 * T), F32)
        accum = jnp.zeros((8, 2 * T), F32)
        for r in range(0, 4 * T, R):
            e = jnp.exp2(ss[r : r + R] - top)
            ss[r : r + R] = e
            total = total + fold(e, jnp.add)
            accum = accum + fold(e * sp[r : r + R], jnp.add)
        total = total.sum(axis=0, keepdims=True)
        accum = accum.sum(axis=0, keepdims=True)
        inverse = 1.0 / total
        delta = accum / total
        lse = top + jnp.log2(total)
        st[0, g, 0:1, :] = lse[:, :T]
        st[0, g, 1:2, :] = lse[:, T:]
        st[0, g, 2:3, :] = delta[:, :T]
        st[0, g, 3:4, :] = delta[:, T:]
        for s in range(4):
            low = [jnp.zeros((8, T), F32) for _ in range(2)]
            high = [jnp.zeros((8, T), F32) for _ in range(2)]
            for r in range(s * T, s * T + T, R):
                p = ss[r : r + R] * inverse
                ds = p * (sp[r : r + R] - delta)
                dsb[g, r : r + R] = ds.astype(BF16)
                if s == 0:
                    pb[g, r : r + R] = p.astype(BF16)
                for j in range(R // 8):
                    a = (r - s * T) // 8 + j
                    for h in range(2):
                        x = ds[8 * j : 8 * j + 8, h * T : h * T + T]
                        if a:
                            x = pltpu.roll(x, T - 8 * a, 1)
                            here = lane8 < T - 8 * a
                            high[h] = high[h] + jnp.where(here, x, 0.0)
                            low[h] = low[h] + jnp.where(here, 0.0, x)
                        else:
                            high[h] = high[h] + x
            for h in range(2):
                both = jnp.concatenate([low[h], high[h]], axis=1)
                for by in (1, 2, 4):
                    both = both + pltpu.roll(pltpu.roll(both, 2 * T - by, 1), 8 - by, 0)
                dgb[s, pl.ds(2 * g + h, 1), :] = both[0:1]

    def st_start(g):
        for s in (1, 2, 3):
            pl.when(me >= s)(lambda s=s: st_copy(s, g).start())

    def query_grads(g):
        q2, do2 = qd[g, 0:T, 0:W], qd[g, 0:T, W : 2 * W]
        turned = dot_nn(kv[g, :, 0:W].T, dsb[g])
        joined = jnp.concatenate([turned[0:64, 0:T], turned[64:T, T : 2 * T]], axis=0)
        dq_ref[:, pl.ds(g * W, W)] = (joined.T * scale).astype(BF16)
        dv0b[g] = jnp.where(first, dot_nn(pb[g, :, 0:T], do2), dot_nn(pb[g, :, T : 2 * T], do2))
        dk0b[g] = jnp.where(first, dot_nn(dsb[g, 0:T, 0:T], q2), dot_nn(dsb[g, 0:T, T : 2 * T], q2))

    def key_side(g):
        qs, dos = qd[g, T : 4 * T, 0:W], qd[g, T : 4 * T, W : 2 * W]
        ks[...] = dot_nt(two(kv[g, 0:T, 0:W]), qs)
        kp[...] = dot_nt(two(kv[g, 0:T, W : 2 * W]), dos)
        for h in range(2):
            for s in (1, 2, 3):
                lse = st[s, g, h : h + 1, :]
                delta = st[s, g, 2 + h : 3 + h, :]
                cols = slice((s - 1) * T, s * T)
                for r in range(h * T, h * T + T, R):
                    x = ks[r : r + R, cols] * c + biask[g, r : r + R, cols]
                    p = jnp.exp2(x - lse)
                    ds = p * (kp[r : r + R, cols] - delta)
                    kpb[r : r + R, cols] = p.astype(BF16)
                    kdsb[r : r + R, cols] = ds.astype(BF16)
        dv_ref[:, pl.ds(g * W, W)] = (merged(dot_nn(kpb[...], dos)) + dv0b[g]).astype(BF16)
        dk_ref[:, pl.ds(g * W, W)] = ((merged(dot_nn(kdsb[...], qs)) + dk0b[g]) * scale).astype(BF16)

    def key_ready(part):
        chunks = pl.ds(part * half, half)
        for s in (1, 3):
            pl.when(after >= s)(lambda s=s: all_of(qd.at[chunks, pl.ds(s * T, T)], qd_far.at[s // 2, part]))
        for s in (1, 2, 3):
            pl.when(after >= s)(lambda s=s: all_of(st.at[s, chunks], st_recv.at[s - 1, part]))

    def keys(start, stop):
        def one(g, carry):
            key_side(g)
            return carry

        lax.fori_loop(start, stop, one, 0)

    def step(g, carry):
        with jax.named_scope("relay"):
            pl.when(g + RELAY < groups)(lambda: kv_relay(g + RELAY))
            pl.when(g + AHEAD < groups)(lambda: send_own(g + AHEAD))
            qd_relay(g)
        with jax.named_scope("kv_wait"):
            kv_arrived(3, g)
            kv_arrived(1, g)
        with jax.named_scope("query"):
            query_scores(g)
            st_start(g)

        @pl.when(g < groups - DEFER)
        def _():
            with jax.named_scope("grads"):
                query_grads(g)

        return carry

    lax.fori_loop(0, groups - 1, step, 0)
    qd_relay(groups - 1)
    with jax.named_scope("kv_wait"):
        kv_arrived(3, groups - 1)
        kv_arrived(1, groups - 1)
    with jax.named_scope("query"):
        query_scores(groups - 1)

    part = jnp.zeros((heads, T), F32)
    with jax.named_scope("buckets"):
        for s in range(4):
            part = part + whole(dot_nt(thirds(pltpu.roll(dgb[s], 2 * T - 1, 1)), onehot(0, s)))
    xpart[...] = part

    def pair_copy():
        return remote(xpart, xpair, sum_send.at[3], sum_recv.at[3], {"seq": partner})

    def result_copy():
        return remote(gbuf, gbuf, sum_send.at[4], sum_recv.at[4], {"seq": partner})

    def x_copy(t):
        return remote(xbuf.at[x_at], xbuf.at[x_at], sum_send.at[0], sum_recv.at[0], x_partner(t))

    def y_copy(t):
        return remote(ybuf.at[y_at], ybuf.at[y_at], sum_send.at[1], sum_recv.at[1], y_partner(t))

    def z_copy(t):
        return remote(zbuf.at[in_z], zbuf.at[in_z], sum_send.at[2], sum_recv.at[2], z_partner(t))

    def total_of(buf, slots):
        return functools.reduce(jnp.add, [buf[i] for i in slots])

    @pl.when(core == 0)
    def _():
        pair_copy().start()

    @pl.when(core == 1)
    def _():
        with jax.named_scope("sum_pair"):
            pair_copy().wait_recv()
            xbuf[x_at] = xpair[...] + xpart[...]
        for t in far_first(nx):
            x_copy(t).start()

    with jax.named_scope("grads"):
        st_start(groups - 1)

        def late(g, carry):
            query_grads(g)
            return carry

        lax.fori_loop(groups - DEFER, groups, late, 0)

    @pl.when(core == 1)
    def _():
        with jax.named_scope("sum_x"):
            all_of(xbuf.at[pl.ds(0, nx - 1)], sum_recv.at[0])
            ybuf[y_at] = total_of(xbuf, range(nx))
        for t in far_first(ny):
            y_copy(t).start()

    with jax.named_scope("build_key"):
        lax.fori_loop(0, groups, build_key, 0)

    @pl.when(core == 1)
    def _():
        with jax.named_scope("sum_y"):
            if ny > 1:
                all_of(ybuf.at[pl.ds(0, ny - 1)], sum_recv.at[1])
            zbuf[in_z] = total_of(ybuf, range(ny))
        for t in far_first(ring_z):
            z_copy(t).start()

    with jax.named_scope("key_wait"):
        key_ready(0)
    with jax.named_scope("key"):
        keys(0, 2)
    with jax.named_scope("key_wait"):
        key_ready(1)
    with jax.named_scope("key"):
        keys(2, LAST_KEY)

    @pl.when(core == 1)
    def _():
        with jax.named_scope("sum_z"):
            all_of(zbuf.at[pl.ds(0, ring_z - 1)], sum_recv.at[2])
        for h in range(n_head):
            gbuf[h * heads : (h + 1) * heads] = total_of(zbuf, range(h * nz, h * nz + nz))
        result_copy().start()

    with jax.named_scope("key"):
        keys(LAST_KEY, groups)

    @pl.when(core == 0)
    def _():
        with jax.named_scope("sum_z"):
            result_copy().wait_recv()

    gb_ref[...] = gbuf[...]

    with jax.named_scope("drain"):
        for n in range(3):
            pl.when(kv_sent[n])(lambda n=n: all_of(kv.at[:, pl.ds(0, T)], kv_send.at[n]))
            pl.when(qd_sent[n])(lambda n=n: all_of(qd.at[:, pl.ds(0, T)], qd_send.at[n]))
        for s in (1, 2, 3):

            @pl.when(me >= s)
            def _():
                all_of(st.at[0], st_send.at[s - 1])
                id_copy(s).wait_send()
                mask_copy(s).wait_send()

        @pl.when(core == 0)
        def _():
            pair_copy().wait_send()

        @pl.when(core == 1)
        def _():
            all_of(xbuf.at[pl.ds(0, nx - 1)], sum_send.at[0])
            if ny > 1:
                all_of(ybuf.at[pl.ds(0, ny - 1)], sum_send.at[1])
            all_of(zbuf.at[pl.ds(0, ring_z - 1)], sum_send.at[2])
            result_copy().wait_send()


def put_out(*refs):
    sems = refs[8]
    copies = [pltpu.make_async_copy(refs[i], refs[4 + i], sems.at[i]) for i in range(4)]
    for copy in copies:
        copy.start()
    for copy in copies:
        copy.wait()


def solution(mesh):
    n_seq, n_head = mesh.shape["seq"], mesh.shape["head"]
    nx, ny, nz = (4, 4, 4) if n_seq == 128 else (2, 1, 2)

    def body(queries, keys, values, grad_out, bias_table, bucket_ids, block_mask):
        tok, width = queries.shape
        heads, buckets = bias_table.shape
        groups = width // 128
        sizes = (n_seq, nx, ny, nz, n_head, heads, groups)
        operands = (queries, keys, values, grad_out, bias_table, bucket_ids, block_mask)
        V = pltpu.VMEM
        dma = pltpu.SemaphoreType.DMA
        scratch = [
            V((groups, 512, 256), BF16), V((groups, 512, 256), BF16),
            V((heads, 128), F32), V((4, 4, 256), jnp.int32), V((4, 1, 4), jnp.int32),
            V((7, heads, 256), F32), V((groups, 512, 256), F32), V((groups, 256, 384), F32),
            V((512, 256), F32), V((512, 256), F32), V((groups, 512, 256), BF16), V((groups, 128, 256), BF16),
            V((256, 384), F32), V((256, 384), F32), V((256, 384), BF16), V((256, 384), BF16),
            V((groups, 128, 128), F32), V((groups, 128, 128), F32),
            V((4, groups, 8, 128), F32), V((4, heads, 256), F32),
            V((heads, 128), F32), V((heads, 128), F32), V((nx, heads, 128), F32), V((ny, heads, 128), F32),
            V((n_head * nz, heads, 128), F32), V((n_head * heads, 128), F32),
            dma((2, 2)), dma((3,)), dma((3,)), dma((3, groups)), dma((3,)), dma((groups,)), dma((2, 2)),
            dma((3,)), dma((3, 2)), dma((2, 3)), dma((2, 3)), dma((5,)), dma((5,)),
        ]
        in_hbm = pl.BlockSpec(memory_space=pltpu.HBM)
        in_vmem = pl.BlockSpec(memory_space=pltpu.VMEM)
        out = jax.ShapeDtypeStruct((tok, width), BF16)
        shapes = (out, out, out, jax.ShapeDtypeStruct((n_head * heads, buckets), F32))
        results = pl.pallas_call(
            functools.partial(kernel, sizes),
            out_shape=shapes,
            in_specs=[in_hbm] * 7,
            out_specs=(in_vmem,) * 4,
            scratch_shapes=scratch,
            compiler_params=pltpu.CompilerParams(
                collective_id=0, has_side_effects=True, vmem_limit_bytes=48 * 1024 * 1024
            ),
        )(*(pltpu.with_memory_space_constraint(x, pltpu.HBM) for x in operands))
        return pl.pallas_call(
            put_out,
            out_shape=shapes,
            in_specs=[in_vmem] * 4,
            out_specs=(pl.BlockSpec(memory_space=pltpu.HBM),) * 4,
            scratch_shapes=[dma((4,))],
        )(*(pltpu.with_memory_space_constraint(x, pltpu.VMEM) for x in results))

    block = P("seq", "head")
    return jax.shard_map(
        body,
        mesh=mesh,
        in_specs=(block, block, block, block, P("head", None), P("seq", None, None), P("seq", None)),
        out_specs=(block, block, block, P(None, None)),
        check_vma=False,
    )
```

```python
import functools

import jax
import jax.numpy as jnp
from jax import lax
from jax.experimental import pallas as pl
from jax.experimental.pallas import tpu as pltpu
from jax.sharding import PartitionSpec as P

MESH = pl.DeviceIdType.MESH
LOG2E = 1.4426950408889634
NEG = -1e30
F32 = jnp.float32
BF16 = jnp.bfloat16
AHEAD = 5
RELAY = 2
FIRST = 3
DEFER = 4
LAST_KEY = 6
NT = (((1,), (1,)), ((), ()))


def dot_nt(a, b, **kw):
    return lax.dot_general(a, b, NT, preferred_element_type=F32, **kw)


def dot_nn(a, b, **kw):
    return jnp.dot(a, b, preferred_element_type=F32, **kw)


def kernel(
    sizes,
    q_hbm, k_hbm, v_hbm, do_hbm, table_hbm, ids_hbm, mask_hbm,
    dq_ref, dk_ref, dv_ref, gb_ref,
    kv, qd, tableb, idsb, maskb, byb, biasq, biask,
    ss, sp, dsb, pb, ks, kp, kpb, kdsb, dk0b, dv0b, st, dgb,
    xpart, xpair, xbuf, ybuf, zbuf, gbuf,
    load_sem, small_sem, kv_send, kv_recv, qd_send, qd_mid, qd_far,
    st_send, st_recv, id_send, id_recv, sum_send, sum_recv,
):
    n_seq, nx, ny, nz, n_head, heads, groups = sizes
    T, W = 128, 128
    half = groups // 2
    scale = 0.125
    c = scale * LOG2E
    me = lax.axis_index("seq")
    hi = lax.axis_index("head")
    core = lax.rem(me, 2)
    partner = me + 1 - 2 * core

    def at(offset):
        return lax.rem(me + (offset + n_seq), n_seq)

    row = 2 * nx
    x_at = lax.rem(me, row) // 2
    y_at = lax.rem(me // row, ny)
    z_at = me // (row * ny)
    ring_z = n_head * nz
    in_z = hi * nz + z_at

    def x_partner(t):
        return {"seq": me + 2 * (lax.rem(x_at + t, nx) - x_at)}

    def y_partner(t):
        return {"seq": me + row * (lax.rem(y_at + t, ny) - y_at)}

    def z_partner(t):
        w = lax.rem(in_z + t, ring_z)
        return {"seq": me + row * ny * (lax.rem(w, nz) - z_at), "head": w // nz}

    def far_first(count):
        return sorted(range(1, count), key=lambda t: -min(t, count - t))

    barrier = pltpu.get_barrier_semaphore()

    def signal(other):
        pl.semaphore_signal(barrier, inc=1, device_id=other, device_id_type=MESH)

    def all_of(ref, sem):
        pltpu.make_async_copy(ref, ref, sem).wait()

    srcs = ((k_hbm, kv, 0, 0), (v_hbm, kv, W, 0), (q_hbm, qd, 0, 1), (do_hbm, qd, W, 1))

    def load(chunks, part):
        for g in chunks:
            for src, dst, off, n in srcs:
                pltpu.make_async_copy(
                    src.at[:, pl.ds(g * W, W)], dst.at[g, pl.ds(0, T), pl.ds(off, W)], load_sem.at[part, n]
                ).start()

    def loaded(start, count, part):
        for n, buf in enumerate((kv, qd)):
            all_of(buf.at[pl.ds(start, count), pl.ds(0, T)], load_sem.at[part, n])

    load(range(FIRST), 0)

    @pl.when(core == 1)
    def _():
        for t in far_first(ring_z):
            signal(z_partner(t))

    small = [
        pltpu.make_async_copy(table_hbm, tableb, small_sem.at[0]),
        pltpu.make_async_copy(ids_hbm.at[0], idsb.at[0], small_sem.at[1]),
        pltpu.make_async_copy(mask_hbm, maskb.at[0], small_sem.at[2]),
    ]
    for copy in small:
        copy.start()

    @pl.when(core == 1)
    def _():
        for t in far_first(ny):
            signal(y_partner(t))
        for t in far_first(nx):
            signal(x_partner(t))

    near = jnp.minimum(me, 3) + jnp.minimum(n_seq - 1 - me, 3)
    for o in (3, 2, 1):
        pl.when(me >= o)(lambda o=o: signal({"seq": me - o}))
        pl.when(me + o < n_seq)(lambda o=o: signal({"seq": me + o}))

    def remote(src, dst, send, recv, device):
        return pltpu.make_async_remote_copy(
            src_ref=src, dst_ref=dst, send_sem=send, recv_sem=recv, device_id=device, device_id_type=MESH
        )

    def slot(buf, g, s):
        return buf.at[g, pl.ds(s * T, T)]

    def kv_copy(n, g):
        if n == 0:
            src, s, device = slot(kv, g, 0), 2, at(2)
        elif n == 1:
            src, s, device = slot(kv, g, 2), 3, at(1)
        else:
            src, s, device = slot(kv, g, pl.multiple_of(2 * core, 2)), 1, partner
        return remote(src, slot(kv, g, s), kv_send.at[n], kv_recv.at[s - 1, g], {"seq": device})

    def qd_copy(n, g):
        if n == 0:
            src, s, device = slot(qd, g, 0), 2, at(-2)
        elif n == 1:
            src, s, device = slot(qd, g, 2), 3, at(-1)
        else:
            src, s, device = slot(qd, g, pl.multiple_of(2 - 2 * core, 2)), 1, partner
        recv = qd_mid.at[g] if s == 2 else qd_far.at[s // 2, g // half]
        return remote(src, slot(qd, g, s), qd_send.at[n], recv, {"seq": device})

    after = n_seq - 1 - me
    kv_sent = (after >= 2, jnp.logical_and(me >= 2, after >= 1), jnp.logical_or(core == 0, me >= 2))
    qd_sent = (me >= 2, jnp.logical_and(after >= 2, me >= 1), jnp.logical_or(core == 1, after >= 2))
    by_slot = {1: 2, 2: 0, 3: 1}

    def kv_start(n, g):
        pl.when(kv_sent[n])(lambda: kv_copy(n, g).start())

    def qd_start(n, g):
        pl.when(qd_sent[n])(lambda: qd_copy(n, g).start())

    def kv_arrived(s, g):
        pl.when(me >= s)(lambda: kv_copy(by_slot[s], g).wait_recv())

    def qd_arrived(g):
        pl.when(after >= 2)(lambda: qd_copy(0, g).wait_recv())

    def st_copy(s, g):
        return remote(st.at[0, g], st.at[s, g], st_send.at[s - 1], st_recv.at[s - 1, g // half], {"seq": at(-s)})

    def id_copy(s):
        return remote(idsb.at[0], idsb.at[s], id_send.at[0, s - 1], id_recv.at[0, s - 1], {"seq": at(-s)})

    def mask_copy(s):
        return remote(maskb.at[0], maskb.at[s], id_send.at[1, s - 1], id_recv.at[1, s - 1], {"seq": at(-s)})

    def send_own(g):
        kv_start(0, g)
        qd_start(0, g)

    def kv_relay(g):
        kv_arrived(2, g)
        kv_start(1, g)
        kv_start(2, g)

    def qd_relay(g):
        qd_arrived(g)
        qd_start(1, g)
        qd_start(2, g)

    with jax.named_scope("load_wait"):
        loaded(0, FIRST, 0)
        for copy in small:
            copy.wait()
    with jax.named_scope("barrier"):
        pl.semaphore_wait(barrier, near + core * (ring_z + ny + nx - 3))
    for g in range(FIRST):
        send_own(g)
        if g == 0:
            for s in (1, 2, 3):

                @pl.when(me >= s)
                def _():
                    id_copy(s).start()
                    mask_copy(s).start()

    load(range(FIRST, groups), 1)
    for s in (1, 2, 3):

        @pl.when(me < s)
        def _():
            kv[:, pl.ds(s * T, T), :] = jnp.zeros((groups, T, 2 * W), BF16)

        @pl.when(after < s)
        def _():
            qd[:, pl.ds(s * T, T), :] = jnp.zeros((groups, T, 2 * W), BF16)
            st[s] = jnp.zeros((groups, 8, T), F32)
            idsb[s] = jnp.zeros((4, 2 * T), jnp.int32)
            maskb[s] = jnp.zeros((1, 4), jnp.int32)

    lane = lax.broadcasted_iota(jnp.int32, (T, T), 1)
    first = lane < 64
    lane8 = lax.broadcasted_iota(jnp.int32, (8, T), 1)
    sub8 = lax.broadcasted_iota(jnp.int32, (8, T), 0)
    codes = lax.broadcasted_iota(jnp.int32, (T, 2 * T), 0)

    def onehot(place, s):
        return (codes == idsb[place, s : s + 1, :]).astype(BF16)

    def thirds(x):
        big = x.astype(BF16)
        rest = x - big.astype(F32)
        mid = rest.astype(BF16)
        return jnp.concatenate([big, mid, (rest - mid.astype(F32)).astype(BF16)], axis=0)

    def whole(x):
        n = x.shape[0] // 3
        return x[:n] + x[n : 2 * n] + x[2 * n :]

    def by_offset(place, s, inside):
        by = whole(dot_nn(thirds(tableb[...] * LOG2E), onehot(place, s)))
        if s:
            keep = jnp.logical_and(maskb[place, 0:1, s : s + 1] == 1, inside)
            by = jnp.where(keep, by, NEG)
        return pltpu.roll(by, 1, 1)

    def skewed(index, head):
        line = jnp.broadcast_to(byb[index, pl.ds(head, 1), :], (8, 2 * T))
        base = pltpu.roll(line, 0, 1, stride=1, stride_axis=0)
        return base[:, :T], base[:, T:]

    def block_row(low, high, a):
        mixed = jnp.where(lane8 >= T - 8 * a, low, high)
        return pltpu.roll(mixed, 8 * a, 1) if a else mixed

    with jax.named_scope("by"):
        for s in range(4):
            byb[s] = by_offset(0, s, me >= s)

    def build_query(g, carry):
        for h in range(2):
            for s in range(4):
                low, high = skewed(s, 2 * g + h)
                for a in range(16):
                    x = block_row(low, high, a)
                    if s == 0:
                        x = jnp.where(8 * a + sub8 <= lane8, x, NEG)
                    biasq[g, pl.ds(s * T + 8 * a, 8), pl.ds(h * T, T)] = x
        return carry

    with jax.named_scope("build_query"):
        lax.fori_loop(0, groups, build_query, 0)
    loaded(FIRST, groups - FIRST, 1)
    send_own(FIRST)
    with jax.named_scope("relay_first"):
        for g in range(RELAY):
            kv_relay(g)
            if FIRST + 1 + g < AHEAD:
                send_own(FIRST + 1 + g)

    def build_key(g, carry):
        for h in range(2):
            for s in (1, 2, 3):
                low, high = skewed(3 + s, 2 * g + h)
                for a in range(16):
                    biask[g, pl.ds(h * T + 8 * a, 8), pl.ds((s - 1) * T, T)] = block_row(low, high, a)
        return carry

    with jax.named_scope("by_key"):
        for s in (1, 2, 3):

            @pl.when(after >= s)
            def _():
                id_copy(s).wait_recv()
                mask_copy(s).wait_recv()

            byb[3 + s] = by_offset(s, s, after >= s)

    def two(x):
        zero = jnp.zeros_like(x)
        return jnp.concatenate([jnp.where(first, x, zero), jnp.where(first, zero, x)], axis=0)

    def merged(x):
        return jnp.where(first, x[:T], x[T:])

    R = 32

    def fold(x, op):
        parts = [x[8 * j : 8 * j + 8] for j in range(x.shape[0] // 8)]
        return functools.reduce(op, parts)

    def query_scores(g):
        q2, do2 = qd[g, 0:T, 0:W], qd[g, 0:T, W : 2 * W]
        ss[...] = dot_nt(kv[g, :, 0:W], two(q2))
        sp[...] = dot_nt(kv[g, :, W : 2 * W], two(do2))
        top = jnp.full((8, 2 * T), NEG, F32)
        for r in range(0, 4 * T, R):
            x = ss[r : r + R] * c + biasq[g, r : r + R]
            ss[r : r + R] = x
            top = jnp.maximum(top, fold(x, jnp.maximum))
        top = top.max(axis=0, keepdims=True)
        total = jnp.zeros((8, 2 * T), F32)
        accum = jnp.zeros((8, 2 * T), F32)
        for r in range(0, 4 * T, R):
            e = jnp.exp2(ss[r : r + R] - top)
            ss[r : r + R] = e
            total = total + fold(e, jnp.add)
            accum = accum + fold(e * sp[r : r + R], jnp.add)
        total = total.sum(axis=0, keepdims=True)
        accum = accum.sum(axis=0, keepdims=True)
        inverse = 1.0 / total
        delta = accum / total
        lse = top + jnp.log2(total)
        st[0, g, 0:1, :] = lse[:, :T]
        st[0, g, 1:2, :] = lse[:, T:]
        st[0, g, 2:3, :] = delta[:, :T]
        st[0, g, 3:4, :] = delta[:, T:]
        for s in range(4):
            low = [jnp.zeros((8, T), F32) for _ in range(2)]
            high = [jnp.zeros((8, T), F32) for _ in range(2)]
            for r in range(s * T, s * T + T, R):
                p = ss[r : r + R] * inverse
                ds = p * (sp[r : r + R] - delta)
                dsb[g, r : r + R] = ds.astype(BF16)
                if s == 0:
                    pb[g, r : r + R] = p.astype(BF16)
                for j in range(R // 8):
                    a = (r - s * T) // 8 + j
                    for h in range(2):
                        x = ds[8 * j : 8 * j + 8, h * T : h * T + T]
                        if a:
                            x = pltpu.roll(x, T - 8 * a, 1)
                            here = lane8 < T - 8 * a
                            high[h] = high[h] + jnp.where(here, x, 0.0)
                            low[h] = low[h] + jnp.where(here, 0.0, x)
                        else:
                            high[h] = high[h] + x
            for h in range(2):
                both = jnp.concatenate([low[h], high[h]], axis=1)
                for by in (1, 2, 4):
                    both = both + pltpu.roll(pltpu.roll(both, 2 * T - by, 1), 8 - by, 0)
                dgb[s, pl.ds(2 * g + h, 1), :] = both[0:1]

    def st_start(g):
        for s in (1, 2, 3):
            pl.when(me >= s)(lambda s=s: st_copy(s, g).start())

    def query_grads(g):
        q2, do2 = qd[g, 0:T, 0:W], qd[g, 0:T, W : 2 * W]
        turned = dot_nn(kv[g, :, 0:W].T, dsb[g])
        joined = jnp.concatenate([turned[0:64, 0:T], turned[64:T, T : 2 * T]], axis=0)
        dq_ref[:, pl.ds(g * W, W)] = (joined.T * scale).astype(BF16)
        dv0b[g] = jnp.where(first, dot_nn(pb[g, :, 0:T], do2), dot_nn(pb[g, :, T : 2 * T], do2))
        dk0b[g] = jnp.where(first, dot_nn(dsb[g, 0:T, 0:T], q2), dot_nn(dsb[g, 0:T, T : 2 * T], q2))

    def key_side(g):
        qs, dos = qd[g, T : 4 * T, 0:W], qd[g, T : 4 * T, W : 2 * W]
        ks[...] = dot_nt(two(kv[g, 0:T, 0:W]), qs)
        kp[...] = dot_nt(two(kv[g, 0:T, W : 2 * W]), dos)
        for h in range(2):
            for s in (1, 2, 3):
                lse = st[s, g, h : h + 1, :]
                delta = st[s, g, 2 + h : 3 + h, :]
                cols = slice((s - 1) * T, s * T)
                for r in range(h * T, h * T + T, R):
                    x = ks[r : r + R, cols] * c + biask[g, r : r + R, cols]
                    p = jnp.exp2(x - lse)
                    ds = p * (kp[r : r + R, cols] - delta)
                    kpb[r : r + R, cols] = p.astype(BF16)
                    kdsb[r : r + R, cols] = ds.astype(BF16)
        dv_ref[:, pl.ds(g * W, W)] = (merged(dot_nn(kpb[...], dos)) + dv0b[g]).astype(BF16)
        dk_ref[:, pl.ds(g * W, W)] = ((merged(dot_nn(kdsb[...], qs)) + dk0b[g]) * scale).astype(BF16)

    def key_ready(part):
        chunks = pl.ds(part * half, half)
        for s in (1, 3):
            pl.when(after >= s)(lambda s=s: all_of(qd.at[chunks, pl.ds(s * T, T)], qd_far.at[s // 2, part]))
        for s in (1, 2, 3):
            pl.when(after >= s)(lambda s=s: all_of(st.at[s, chunks], st_recv.at[s - 1, part]))

    def keys(start, stop):
        def one(g, carry):
            key_side(g)
            return carry

        lax.fori_loop(start, stop, one, 0)

    def step(g, carry):
        with jax.named_scope("relay"):
            pl.when(g + RELAY < groups)(lambda: kv_relay(g + RELAY))
            pl.when(g + AHEAD < groups)(lambda: send_own(g + AHEAD))
            qd_relay(g)
        with jax.named_scope("kv_wait"):
            kv_arrived(3, g)
            kv_arrived(1, g)
        with jax.named_scope("query"):
            query_scores(g)
            st_start(g)

        @pl.when(g < groups - DEFER)
        def _():
            with jax.named_scope("grads"):
                query_grads(g)

        return carry

    lax.fori_loop(0, groups - 1, step, 0)
    qd_relay(groups - 1)
    with jax.named_scope("kv_wait"):
        kv_arrived(3, groups - 1)
        kv_arrived(1, groups - 1)
    with jax.named_scope("query"):
        query_scores(groups - 1)

    part = jnp.zeros((heads, T), F32)
    with jax.named_scope("buckets"):
        for s in range(4):
            part = part + whole(dot_nt(thirds(pltpu.roll(dgb[s], 2 * T - 1, 1)), onehot(0, s)))
    xpart[...] = part

    def pair_copy():
        return remote(xpart, xpair, sum_send.at[3], sum_recv.at[3], {"seq": partner})

    def result_copy():
        return remote(gbuf, gbuf, sum_send.at[4], sum_recv.at[4], {"seq": partner})

    def x_copy(t):
        return remote(xbuf.at[x_at], xbuf.at[x_at], sum_send.at[0], sum_recv.at[0], x_partner(t))

    def y_copy(t):
        return remote(ybuf.at[y_at], ybuf.at[y_at], sum_send.at[1], sum_recv.at[1], y_partner(t))

    def z_copy(t):
        return remote(zbuf.at[in_z], zbuf.at[in_z], sum_send.at[2], sum_recv.at[2], z_partner(t))

    def total_of(buf, slots):
        return functools.reduce(jnp.add, [buf[i] for i in slots])

    @pl.when(core == 0)
    def _():
        pair_copy().start()

    with jax.named_scope("grads"):
        st_start(groups - 1)

        def late(g, carry):
            query_grads(g)
            return carry

        lax.fori_loop(groups - DEFER, groups, late, 0)

    @pl.when(core == 1)
    def _():
        with jax.named_scope("sum_pair"):
            pair_copy().wait_recv()
            xbuf[x_at] = xpair[...] + xpart[...]
        for t in far_first(nx):
            x_copy(t).start()

    with jax.named_scope("build_key"):
        lax.fori_loop(0, groups - 2, build_key, 0)

    @pl.when(core == 1)
    def _():
        with jax.named_scope("sum_x"):
            all_of(xbuf.at[pl.ds(0, nx - 1)], sum_recv.at[0])
            ybuf[y_at] = total_of(xbuf, range(nx))
        for t in far_first(ny):
            y_copy(t).start()

    with jax.named_scope("build_key"):
        lax.fori_loop(groups - 2, groups, build_key, 0)
    with jax.named_scope("key_wait"):
        key_ready(0)
    with jax.named_scope("key"):
        keys(0, 2)

    @pl.when(core == 1)
    def _():
        with jax.named_scope("sum_y"):
            if ny > 1:
                all_of(ybuf.at[pl.ds(0, ny - 1)], sum_recv.at[1])
            zbuf[in_z] = total_of(ybuf, range(ny))
        for t in far_first(ring_z):
            z_copy(t).start()

    with jax.named_scope("key_wait"):
        key_ready(1)
    with jax.named_scope("key"):
        keys(2, LAST_KEY)

    @pl.when(core == 1)
    def _():
        with jax.named_scope("sum_z"):
            all_of(zbuf.at[pl.ds(0, ring_z - 1)], sum_recv.at[2])
        for h in range(n_head):
            gbuf[h * heads : (h + 1) * heads] = total_of(zbuf, range(h * nz, h * nz + nz))
        result_copy().start()

    with jax.named_scope("key"):
        keys(LAST_KEY, groups)

    @pl.when(core == 0)
    def _():
        with jax.named_scope("sum_z"):
            result_copy().wait_recv()

    gb_ref[...] = gbuf[...]

    with jax.named_scope("drain"):
        for n in range(3):
            pl.when(kv_sent[n])(lambda n=n: all_of(kv.at[:, pl.ds(0, T)], kv_send.at[n]))
            pl.when(qd_sent[n])(lambda n=n: all_of(qd.at[:, pl.ds(0, T)], qd_send.at[n]))
        for s in (1, 2, 3):

            @pl.when(me >= s)
            def _():
                all_of(st.at[0], st_send.at[s - 1])
                id_copy(s).wait_send()
                mask_copy(s).wait_send()

        @pl.when(core == 0)
        def _():
            pair_copy().wait_send()

        @pl.when(core == 1)
        def _():
            all_of(xbuf.at[pl.ds(0, nx - 1)], sum_send.at[0])
            if ny > 1:
                all_of(ybuf.at[pl.ds(0, ny - 1)], sum_send.at[1])
            all_of(zbuf.at[pl.ds(0, ring_z - 1)], sum_send.at[2])
            result_copy().wait_send()


def put_out(*refs):
    sems = refs[8]
    copies = [pltpu.make_async_copy(refs[i], refs[4 + i], sems.at[i]) for i in range(4)]
    for copy in copies:
        copy.start()
    for copy in copies:
        copy.wait()


def solution(mesh):
    n_seq, n_head = mesh.shape["seq"], mesh.shape["head"]
    nx, ny, nz = (4, 4, 4) if n_seq == 128 else (2, 1, 2)

    def body(queries, keys, values, grad_out, bias_table, bucket_ids, block_mask):
        tok, width = queries.shape
        heads, buckets = bias_table.shape
        groups = width // 128
        sizes = (n_seq, nx, ny, nz, n_head, heads, groups)
        operands = (queries, keys, values, grad_out, bias_table, bucket_ids, block_mask)
        V = pltpu.VMEM
        dma = pltpu.SemaphoreType.DMA
        scratch = [
            V((groups, 512, 256), BF16), V((groups, 512, 256), BF16),
            V((heads, 128), F32), V((4, 4, 256), jnp.int32), V((4, 1, 4), jnp.int32),
            V((7, heads, 256), F32), V((groups, 512, 256), F32), V((groups, 256, 384), F32),
            V((512, 256), F32), V((512, 256), F32), V((groups, 512, 256), BF16), V((groups, 128, 256), BF16),
            V((256, 384), F32), V((256, 384), F32), V((256, 384), BF16), V((256, 384), BF16),
            V((groups, 128, 128), F32), V((groups, 128, 128), F32),
            V((4, groups, 8, 128), F32), V((4, heads, 256), F32),
            V((heads, 128), F32), V((heads, 128), F32), V((nx, heads, 128), F32), V((ny, heads, 128), F32),
            V((n_head * nz, heads, 128), F32), V((n_head * heads, 128), F32),
            dma((2, 2)), dma((3,)), dma((3,)), dma((3, groups)), dma((3,)), dma((groups,)), dma((2, 2)),
            dma((3,)), dma((3, 2)), dma((2, 3)), dma((2, 3)), dma((5,)), dma((5,)),
        ]
        in_hbm = pl.BlockSpec(memory_space=pltpu.HBM)
        in_vmem = pl.BlockSpec(memory_space=pltpu.VMEM)
        out = jax.ShapeDtypeStruct((tok, width), BF16)
        shapes = (out, out, out, jax.ShapeDtypeStruct((n_head * heads, buckets), F32))
        results = pl.pallas_call(
            functools.partial(kernel, sizes),
            out_shape=shapes,
            in_specs=[in_hbm] * 7,
            out_specs=(in_vmem,) * 4,
            scratch_shapes=scratch,
            compiler_params=pltpu.CompilerParams(
                collective_id=0, has_side_effects=True, vmem_limit_bytes=48 * 1024 * 1024
            ),
        )(*(pltpu.with_memory_space_constraint(x, pltpu.HBM) for x in operands))
        return pl.pallas_call(
            put_out,
            out_shape=shapes,
            in_specs=[in_vmem] * 4,
            out_specs=(pl.BlockSpec(memory_space=pltpu.HBM),) * 4,
            scratch_shapes=[dma((4,))],
        )(*(pltpu.with_memory_space_constraint(x, pltpu.VMEM) for x in results))

    block = P("seq", "head")
    return jax.shard_map(
        body,
        mesh=mesh,
        in_specs=(block, block, block, block, P("head", None), P("seq", None, None), P("seq", None)),
        out_specs=(block, block, block, P(None, None)),
        check_vma=False,
    )
```

```python
import functools

import jax
import jax.numpy as jnp
from jax import lax
from jax.experimental import pallas as pl
from jax.experimental.pallas import tpu as pltpu
from jax.sharding import PartitionSpec as P

MESH = pl.DeviceIdType.MESH
LOG2E = 1.4426950408889634
NEG = -1e30
F32 = jnp.float32
BF16 = jnp.bfloat16
AHEAD = 5
RELAY = 2
FIRST = 3
DEFER = 4
LAST_KEY = 6
PIECES = 4
NT = (((1,), (1,)), ((), ()))


def dot_nt(a, b, **kw):
    return lax.dot_general(a, b, NT, preferred_element_type=F32, **kw)


def dot_nn(a, b, **kw):
    return jnp.dot(a, b, preferred_element_type=F32, **kw)


def kernel(
    sizes,
    q_hbm, k_hbm, v_hbm, do_hbm, table_hbm, ids_hbm, mask_hbm,
    dq_ref, dk_ref, dv_ref, gb_ref,
    kv, qd, tableb, idsb, maskb, byb, biasq, biask,
    ss, sp, dsb, pb, ks, kp, kpb, kdsb, dk0b, dv0b, st, dgb,
    xpart, xpair, xbuf, ybuf, zbuf, gbuf,
    load_sem, small_sem, kv_send, kv_recv, qd_send, qd_mid, qd_far,
    st_send, st_recv, id_send, id_recv, sum_send, sum_recv,
):
    n_seq, nx, ny, nz, n_head, heads, groups = sizes
    T, W = 128, 128
    half = groups // 2
    scale = 0.125
    c = scale * LOG2E
    me = lax.axis_index("seq")
    hi = lax.axis_index("head")
    core = lax.rem(me, 2)
    partner = me + 1 - 2 * core

    def at(offset):
        return lax.rem(me + (offset + n_seq), n_seq)

    row = 2 * nx
    x_at = lax.rem(me, row) // 2
    y_at = lax.rem(me // row, ny)
    z_at = me // (row * ny)
    ring_z = n_head * nz
    in_z = hi * nz + z_at

    def x_partner(t):
        return {"seq": me + 2 * (lax.rem(x_at + t, nx) - x_at)}

    def y_partner(t):
        return {"seq": me + row * (lax.rem(y_at + t, ny) - y_at)}

    def z_partner(t):
        w = lax.rem(in_z + t, ring_z)
        return {"seq": me + row * ny * (lax.rem(w, nz) - z_at), "head": w // nz}

    def far_first(count):
        return sorted(range(1, count), key=lambda t: -min(t, count - t))

    barrier = pltpu.get_barrier_semaphore()

    def signal(other):
        pl.semaphore_signal(barrier, inc=1, device_id=other, device_id_type=MESH)

    def all_of(ref, sem):
        pltpu.make_async_copy(ref, ref, sem).wait()

    srcs = ((k_hbm, kv, 0, 0), (v_hbm, kv, W, 0), (q_hbm, qd, 0, 1), (do_hbm, qd, W, 1))

    def load(chunks, part):
        for g in chunks:
            for src, dst, off, n in srcs:
                pltpu.make_async_copy(
                    src.at[:, pl.ds(g * W, W)], dst.at[g, pl.ds(0, T), pl.ds(off, W)], load_sem.at[part, n]
                ).start()

    def loaded(start, count, part):
        for n, buf in enumerate((kv, qd)):
            all_of(buf.at[pl.ds(start, count), pl.ds(0, T)], load_sem.at[part, n])

    load(range(FIRST), 0)

    @pl.when(core == 1)
    def _():
        for t in far_first(ring_z):
            signal(z_partner(t))

    small = [
        pltpu.make_async_copy(table_hbm, tableb, small_sem.at[0]),
        pltpu.make_async_copy(ids_hbm.at[0], idsb.at[0], small_sem.at[1]),
        pltpu.make_async_copy(mask_hbm, maskb.at[0], small_sem.at[2]),
    ]
    for copy in small:
        copy.start()

    @pl.when(core == 1)
    def _():
        for t in far_first(ny):
            signal(y_partner(t))
        for t in far_first(nx):
            signal(x_partner(t))

    near = jnp.minimum(me, 3) + jnp.minimum(n_seq - 1 - me, 3)
    for o in (3, 2, 1):
        pl.when(me >= o)(lambda o=o: signal({"seq": me - o}))
        pl.when(me + o < n_seq)(lambda o=o: signal({"seq": me + o}))

    def remote(src, dst, send, recv, device):
        return pltpu.make_async_remote_copy(
            src_ref=src, dst_ref=dst, send_sem=send, recv_sem=recv, device_id=device, device_id_type=MESH
        )

    def slot(buf, g, s):
        return buf.at[g, pl.ds(s * T, T)]

    def kv_copy(n, g):
        if n == 0:
            src, s, device = slot(kv, g, 0), 2, at(2)
        elif n == 1:
            src, s, device = slot(kv, g, 2), 3, at(1)
        else:
            src, s, device = slot(kv, g, pl.multiple_of(2 * core, 2)), 1, partner
        return remote(src, slot(kv, g, s), kv_send.at[n], kv_recv.at[s - 1, g], {"seq": device})

    def qd_copy(n, g):
        if n == 0:
            src, s, device = slot(qd, g, 0), 2, at(-2)
        elif n == 1:
            src, s, device = slot(qd, g, 2), 3, at(-1)
        else:
            src, s, device = slot(qd, g, pl.multiple_of(2 - 2 * core, 2)), 1, partner
        recv = qd_mid.at[g] if s == 2 else qd_far.at[s // 2, g // half]
        return remote(src, slot(qd, g, s), qd_send.at[n], recv, {"seq": device})

    after = n_seq - 1 - me
    kv_sent = (after >= 2, jnp.logical_and(me >= 2, after >= 1), jnp.logical_or(core == 0, me >= 2))
    qd_sent = (me >= 2, jnp.logical_and(after >= 2, me >= 1), jnp.logical_or(core == 1, after >= 2))
    by_slot = {1: 2, 2: 0, 3: 1}

    def kv_start(n, g):
        pl.when(kv_sent[n])(lambda: kv_copy(n, g).start())

    def qd_start(n, g):
        pl.when(qd_sent[n])(lambda: qd_copy(n, g).start())

    def kv_arrived(s, g):
        pl.when(me >= s)(lambda: kv_copy(by_slot[s], g).wait_recv())

    def qd_arrived(g):
        pl.when(after >= 2)(lambda: qd_copy(0, g).wait_recv())

    def st_copy(s, g):
        return remote(st.at[0, g], st.at[s, g], st_send.at[s - 1], st_recv.at[s - 1, g // half], {"seq": at(-s)})

    def id_copy(s):
        return remote(idsb.at[0], idsb.at[s], id_send.at[0, s - 1], id_recv.at[0, s - 1], {"seq": at(-s)})

    def mask_copy(s):
        return remote(maskb.at[0], maskb.at[s], id_send.at[1, s - 1], id_recv.at[1, s - 1], {"seq": at(-s)})

    def send_own(g):
        kv_start(0, g)
        qd_start(0, g)

    def kv_relay(g):
        kv_arrived(2, g)
        kv_start(1, g)
        kv_start(2, g)

    def qd_relay(g):
        qd_arrived(g)
        qd_start(1, g)
        qd_start(2, g)

    with jax.named_scope("load_wait"):
        loaded(0, FIRST, 0)
        for copy in small:
            copy.wait()
    with jax.named_scope("barrier"):
        pl.semaphore_wait(barrier, near + core * (ring_z + ny + nx - 3))
    for g in range(FIRST):
        send_own(g)
        if g == 0:
            for s in (1, 2, 3):

                @pl.when(me >= s)
                def _():
                    id_copy(s).start()
                    mask_copy(s).start()

    load(range(FIRST, groups), 1)
    for s in (1, 2, 3):

        @pl.when(me < s)
        def _():
            kv[:, pl.ds(s * T, T), :] = jnp.zeros((groups, T, 2 * W), BF16)

        @pl.when(after < s)
        def _():
            qd[:, pl.ds(s * T, T), :] = jnp.zeros((groups, T, 2 * W), BF16)
            st[s] = jnp.zeros((groups, 8, T), F32)
            idsb[s] = jnp.zeros((4, 2 * T), jnp.int32)
            maskb[s] = jnp.zeros((1, 4), jnp.int32)

    lane = lax.broadcasted_iota(jnp.int32, (T, T), 1)
    first = lane < 64
    lane8 = lax.broadcasted_iota(jnp.int32, (8, T), 1)
    sub8 = lax.broadcasted_iota(jnp.int32, (8, T), 0)
    codes = lax.broadcasted_iota(jnp.int32, (T, 2 * T), 0)

    def onehot(place, s):
        return (codes == idsb[place, s : s + 1, :]).astype(BF16)

    def thirds(x):
        big = x.astype(BF16)
        rest = x - big.astype(F32)
        mid = rest.astype(BF16)
        return jnp.concatenate([big, mid, (rest - mid.astype(F32)).astype(BF16)], axis=0)

    def whole(x):
        n = x.shape[0] // 3
        return x[:n] + x[n : 2 * n] + x[2 * n :]

    def by_offset(place, s, inside):
        by = whole(dot_nn(thirds(tableb[...] * LOG2E), onehot(place, s)))
        if s:
            keep = jnp.logical_and(maskb[place, 0:1, s : s + 1] == 1, inside)
            by = jnp.where(keep, by, NEG)
        return pltpu.roll(by, 1, 1)

    def skewed(index, head):
        line = jnp.broadcast_to(byb[index, pl.ds(head, 1), :], (8, 2 * T))
        base = pltpu.roll(line, 0, 1, stride=1, stride_axis=0)
        return base[:, :T], base[:, T:]

    def block_row(low, high, a):
        mixed = jnp.where(lane8 >= T - 8 * a, low, high)
        return pltpu.roll(mixed, 8 * a, 1) if a else mixed

    with jax.named_scope("by"):
        for s in range(4):
            byb[s] = by_offset(0, s, me >= s)

    def build_query(g, carry):
        for h in range(2):
            for s in range(4):
                low, high = skewed(s, 2 * g + h)
                for a in range(16):
                    x = block_row(low, high, a)
                    if s == 0:
                        x = jnp.where(8 * a + sub8 <= lane8, x, NEG)
                    biasq[g, pl.ds(s * T + 8 * a, 8), pl.ds(h * T, T)] = x
        return carry

    with jax.named_scope("build_query"):
        lax.fori_loop(0, groups, build_query, 0)
    loaded(FIRST, groups - FIRST, 1)
    send_own(FIRST)
    with jax.named_scope("relay_first"):
        for g in range(RELAY):
            kv_relay(g)
            if FIRST + 1 + g < AHEAD:
                send_own(FIRST + 1 + g)

    def build_key(g, carry):
        for h in range(2):
            for s in (1, 2, 3):
                low, high = skewed(3 + s, 2 * g + h)
                for a in range(16):
                    biask[g, pl.ds(h * T + 8 * a, 8), pl.ds((s - 1) * T, T)] = block_row(low, high, a)
        return carry

    with jax.named_scope("by_key"):
        for s in (1, 2, 3):

            @pl.when(after >= s)
            def _():
                id_copy(s).wait_recv()
                mask_copy(s).wait_recv()

            byb[3 + s] = by_offset(s, s, after >= s)

    def two(x):
        zero = jnp.zeros_like(x)
        return jnp.concatenate([jnp.where(first, x, zero), jnp.where(first, zero, x)], axis=0)

    def merged(x):
        return jnp.where(first, x[:T], x[T:])

    R = 32

    def fold(x, op):
        parts = [x[8 * j : 8 * j + 8] for j in range(x.shape[0] // 8)]
        return functools.reduce(op, parts)

    def query_scores(g):
        q2, do2 = qd[g, 0:T, 0:W], qd[g, 0:T, W : 2 * W]
        ss[...] = dot_nt(kv[g, :, 0:W], two(q2))
        sp[...] = dot_nt(kv[g, :, W : 2 * W], two(do2))
        top = jnp.full((8, 2 * T), NEG, F32)
        for r in range(0, 4 * T, R):
            x = ss[r : r + R] * c + biasq[g, r : r + R]
            ss[r : r + R] = x
            top = jnp.maximum(top, fold(x, jnp.maximum))
        top = top.max(axis=0, keepdims=True)
        total = jnp.zeros((8, 2 * T), F32)
        accum = jnp.zeros((8, 2 * T), F32)
        for r in range(0, 4 * T, R):
            e = jnp.exp2(ss[r : r + R] - top)
            ss[r : r + R] = e
            total = total + fold(e, jnp.add)
            accum = accum + fold(e * sp[r : r + R], jnp.add)
        total = total.sum(axis=0, keepdims=True)
        accum = accum.sum(axis=0, keepdims=True)
        inverse = 1.0 / total
        delta = accum / total
        lse = top + jnp.log2(total)
        st[0, g, 0:1, :] = lse[:, :T]
        st[0, g, 1:2, :] = lse[:, T:]
        st[0, g, 2:3, :] = delta[:, :T]
        st[0, g, 3:4, :] = delta[:, T:]
        for s in range(4):
            low = [jnp.zeros((8, T), F32) for _ in range(2)]
            high = [jnp.zeros((8, T), F32) for _ in range(2)]
            for r in range(s * T, s * T + T, R):
                p = ss[r : r + R] * inverse
                ds = p * (sp[r : r + R] - delta)
                dsb[g, r : r + R] = ds.astype(BF16)
                if s == 0:
                    pb[g, r : r + R] = p.astype(BF16)
                for j in range(R // 8):
                    a = (r - s * T) // 8 + j
                    for h in range(2):
                        x = ds[8 * j : 8 * j + 8, h * T : h * T + T]
                        if a:
                            x = pltpu.roll(x, T - 8 * a, 1)
                            here = lane8 < T - 8 * a
                            high[h] = high[h] + jnp.where(here, x, 0.0)
                            low[h] = low[h] + jnp.where(here, 0.0, x)
                        else:
                            high[h] = high[h] + x
            for h in range(2):
                both = jnp.concatenate([low[h], high[h]], axis=1)
                for by in (1, 2, 4):
                    both = both + pltpu.roll(pltpu.roll(both, 2 * T - by, 1), 8 - by, 0)
                dgb[s, pl.ds(2 * g + h, 1), :] = both[0:1]

    def st_start(g):
        for s in (1, 2, 3):
            pl.when(me >= s)(lambda s=s: st_copy(s, g).start())

    def query_grads(g):
        q2, do2 = qd[g, 0:T, 0:W], qd[g, 0:T, W : 2 * W]
        turned = dot_nn(kv[g, :, 0:W].T, dsb[g])
        joined = jnp.concatenate([turned[0:64, 0:T], turned[64:T, T : 2 * T]], axis=0)
        dq_ref[:, pl.ds(g * W, W)] = (joined.T * scale).astype(BF16)
        dv0b[g] = jnp.where(first, dot_nn(pb[g, :, 0:T], do2), dot_nn(pb[g, :, T : 2 * T], do2))
        dk0b[g] = jnp.where(first, dot_nn(dsb[g, 0:T, 0:T], q2), dot_nn(dsb[g, 0:T, T : 2 * T], q2))

    def key_side(g):
        qs, dos = qd[g, T : 4 * T, 0:W], qd[g, T : 4 * T, W : 2 * W]
        ks[...] = dot_nt(two(kv[g, 0:T, 0:W]), qs)
        kp[...] = dot_nt(two(kv[g, 0:T, W : 2 * W]), dos)
        for h in range(2):
            for s in (1, 2, 3):
                lse = st[s, g, h : h + 1, :]
                delta = st[s, g, 2 + h : 3 + h, :]
                cols = slice((s - 1) * T, s * T)
                for r in range(h * T, h * T + T, R):
                    x = ks[r : r + R, cols] * c + biask[g, r : r + R, cols]
                    p = jnp.exp2(x - lse)
                    ds = p * (kp[r : r + R, cols] - delta)
                    kpb[r : r + R, cols] = p.astype(BF16)
                    kdsb[r : r + R, cols] = ds.astype(BF16)
        dv_ref[:, pl.ds(g * W, W)] = (merged(dot_nn(kpb[...], dos)) + dv0b[g]).astype(BF16)
        dk_ref[:, pl.ds(g * W, W)] = ((merged(dot_nn(kdsb[...], qs)) + dk0b[g]) * scale).astype(BF16)

    def key_ready(part):
        chunks = pl.ds(part * half, half)
        for s in (1, 3):
            pl.when(after >= s)(lambda s=s: all_of(qd.at[chunks, pl.ds(s * T, T)], qd_far.at[s // 2, part]))
        for s in (1, 2, 3):
            pl.when(after >= s)(lambda s=s: all_of(st.at[s, chunks], st_recv.at[s - 1, part]))

    def keys(start, stop):
        def one(g, carry):
            key_side(g)
            return carry

        lax.fori_loop(start, stop, one, 0)

    def step(g, carry):
        with jax.named_scope("relay"):
            pl.when(g + RELAY < groups)(lambda: kv_relay(g + RELAY))
            pl.when(g + AHEAD < groups)(lambda: send_own(g + AHEAD))
            qd_relay(g)
        with jax.named_scope("kv_wait"):
            kv_arrived(3, g)
            kv_arrived(1, g)
        with jax.named_scope("query"):
            query_scores(g)
            st_start(g)

        @pl.when(g < groups - DEFER)
        def _():
            with jax.named_scope("grads"):
                query_grads(g)

        return carry

    lax.fori_loop(0, groups - 1, step, 0)
    qd_relay(groups - 1)
    with jax.named_scope("kv_wait"):
        kv_arrived(3, groups - 1)
        kv_arrived(1, groups - 1)
    with jax.named_scope("query"):
        query_scores(groups - 1)

    part = jnp.zeros((heads, T), F32)
    with jax.named_scope("buckets"):
        for s in range(4):
            part = part + whole(dot_nt(thirds(pltpu.roll(dgb[s], 2 * T - 1, 1)), onehot(0, s)))
    xpart[...] = part

    def pair_copy():
        return remote(xpart, xpair, sum_send.at[3], sum_recv.at[3], {"seq": partner})

    def result_copy():
        return remote(gbuf, gbuf, sum_send.at[4], sum_recv.at[4], {"seq": partner})

    def x_copy(t):
        return remote(xbuf.at[x_at], xbuf.at[x_at], sum_send.at[0], sum_recv.at[0], x_partner(t))

    def y_copy(t):
        return remote(ybuf.at[y_at], ybuf.at[y_at], sum_send.at[1], sum_recv.at[1], y_partner(t))

    def z_copy(t):
        return remote(zbuf.at[in_z], zbuf.at[in_z], sum_send.at[2], sum_recv.at[2], z_partner(t))

    def total_of(buf, slots):
        return functools.reduce(jnp.add, [buf[i] for i in slots])

    @pl.when(core == 0)
    def _():
        pair_copy().start()

    with jax.named_scope("grads"):
        st_start(groups - 1)

        def late(g, carry):
            query_grads(g)
            return carry

        lax.fori_loop(groups - DEFER, groups, late, 0)

    @pl.when(core == 1)
    def _():
        with jax.named_scope("sum_pair"):
            pair_copy().wait_recv()
            xbuf[x_at] = xpair[...] + xpart[...]
        for t in far_first(nx):
            x_copy(t).start()

    with jax.named_scope("build_key"):
        lax.fori_loop(0, groups - 2, build_key, 0)

    @pl.when(core == 1)
    def _():
        with jax.named_scope("sum_x"):
            all_of(xbuf.at[pl.ds(0, nx - 1)], sum_recv.at[0])
            ybuf[y_at] = total_of(xbuf, range(nx))
        for t in far_first(ny):
            y_copy(t).start()

    with jax.named_scope("build_key"):
        lax.fori_loop(groups - 2, groups, build_key, 0)
    with jax.named_scope("key_wait"):
        key_ready(0)
    with jax.named_scope("key"):
        keys(0, 2)

    @pl.when(core == 1)
    def _():
        with jax.named_scope("sum_y"):
            if ny > 1:
                all_of(ybuf.at[pl.ds(0, ny - 1)], sum_recv.at[1])
            zbuf[in_z] = total_of(ybuf, range(ny))
        for t in far_first(ring_z):
            z_copy(t).start()

    with jax.named_scope("key_wait"):
        key_ready(1)
    with jax.named_scope("key"):
        keys(2, LAST_KEY)

    @pl.when(core == 1)
    def _():
        with jax.named_scope("sum_z"):
            all_of(zbuf.at[pl.ds(0, ring_z - 1)], sum_recv.at[2])
        for h in range(n_head):
            gbuf[h * heads : (h + 1) * heads] = total_of(zbuf, range(h * nz, h * nz + nz))
        result_copy().start()

    with jax.named_scope("key"):
        keys(LAST_KEY, groups)

    @pl.when(core == 0)
    def _():
        with jax.named_scope("sum_z"):
            result_copy().wait_recv()

    gb_ref[...] = gbuf[...]

    with jax.named_scope("drain"):
        for n in range(3):
            pl.when(kv_sent[n])(lambda n=n: all_of(kv.at[:, pl.ds(0, T)], kv_send.at[n]))
            pl.when(qd_sent[n])(lambda n=n: all_of(qd.at[:, pl.ds(0, T)], qd_send.at[n]))
        for s in (1, 2, 3):

            @pl.when(me >= s)
            def _():
                all_of(st.at[0], st_send.at[s - 1])
                id_copy(s).wait_send()
                mask_copy(s).wait_send()

        @pl.when(core == 0)
        def _():
            pair_copy().wait_send()

        @pl.when(core == 1)
        def _():
            all_of(xbuf.at[pl.ds(0, nx - 1)], sum_send.at[0])
            if ny > 1:
                all_of(ybuf.at[pl.ds(0, ny - 1)], sum_send.at[1])
            all_of(zbuf.at[pl.ds(0, ring_z - 1)], sum_send.at[2])
            result_copy().wait_send()


def put_out(*refs):
    sems = refs[8]
    pieces = [(i, r) for r in range(PIECES) for i in range(3)]
    copies = [pltpu.make_async_copy(refs[3], refs[7], sems.at[3 * PIECES])]
    for n, (i, r) in enumerate(pieces):
        size = refs[i].shape[0] // PIECES
        rows = pl.ds(r * size, size)
        copies.append(pltpu.make_async_copy(refs[i].at[rows], refs[4 + i].at[rows], sems.at[n]))
    for copy in copies:
        copy.start()
    for copy in copies:
        copy.wait()


def solution(mesh):
    n_seq, n_head = mesh.shape["seq"], mesh.shape["head"]
    nx, ny, nz = (4, 4, 4) if n_seq == 128 else (2, 1, 2)

    def body(queries, keys, values, grad_out, bias_table, bucket_ids, block_mask):
        tok, width = queries.shape
        heads, buckets = bias_table.shape
        groups = width // 128
        sizes = (n_seq, nx, ny, nz, n_head, heads, groups)
        operands = (queries, keys, values, grad_out, bias_table, bucket_ids, block_mask)
        V = pltpu.VMEM
        dma = pltpu.SemaphoreType.DMA
        scratch = [
            V((groups, 512, 256), BF16), V((groups, 512, 256), BF16),
            V((heads, 128), F32), V((4, 4, 256), jnp.int32), V((4, 1, 4), jnp.int32),
            V((7, heads, 256), F32), V((groups, 512, 256), F32), V((groups, 256, 384), F32),
            V((512, 256), F32), V((512, 256), F32), V((groups, 512, 256), BF16), V((groups, 128, 256), BF16),
            V((256, 384), F32), V((256, 384), F32), V((256, 384), BF16), V((256, 384), BF16),
            V((groups, 128, 128), F32), V((groups, 128, 128), F32),
            V((4, groups, 8, 128), F32), V((4, heads, 256), F32),
            V((heads, 128), F32), V((heads, 128), F32), V((nx, heads, 128), F32), V((ny, heads, 128), F32),
            V((n_head * nz, heads, 128), F32), V((n_head * heads, 128), F32),
            dma((2, 2)), dma((3,)), dma((3,)), dma((3, groups)), dma((3,)), dma((groups,)), dma((2, 2)),
            dma((3,)), dma((3, 2)), dma((2, 3)), dma((2, 3)), dma((5,)), dma((5,)),
        ]
        in_hbm = pl.BlockSpec(memory_space=pltpu.HBM)
        in_vmem = pl.BlockSpec(memory_space=pltpu.VMEM)
        out = jax.ShapeDtypeStruct((tok, width), BF16)
        shapes = (out, out, out, jax.ShapeDtypeStruct((n_head * heads, buckets), F32))
        results = pl.pallas_call(
            functools.partial(kernel, sizes),
            out_shape=shapes,
            in_specs=[in_hbm] * 7,
            out_specs=(in_vmem,) * 4,
            scratch_shapes=scratch,
            compiler_params=pltpu.CompilerParams(
                collective_id=0, has_side_effects=True, vmem_limit_bytes=48 * 1024 * 1024
            ),
        )(*(pltpu.with_memory_space_constraint(x, pltpu.HBM) for x in operands))
        return pl.pallas_call(
            put_out,
            out_shape=shapes,
            in_specs=[in_vmem] * 4,
            out_specs=(pl.BlockSpec(memory_space=pltpu.HBM),) * 4,
            scratch_shapes=[dma((3 * PIECES + 1,))],
        )(*(pltpu.with_memory_space_constraint(x, pltpu.VMEM) for x in results))

    block = P("seq", "head")
    return jax.shard_map(
        body,
        mesh=mesh,
        in_specs=(block, block, block, block, P("head", None), P("seq", None, None), P("seq", None)),
        out_specs=(block, block, block, P(None, None)),
        check_vma=False,
    )
```
